32 devices in a mesh: rows: 8 (over z, x), grp: 4 (over y, core).
Axes of the slice: x: 2, y: 2, z: 4, core: 2. Of those that a mesh axis runs over, the one named last changes fastest.
Arguments:
- sketch: float32 [2048, 8192], P(None, ('rows', 'grp')), may hold values from -0.125 to 0.125
- prior_basis: float32 [8192, 512], P(('rows', 'grp'))
- panel_block: float32 [8192, 256], P(('rows', 'grp'))
- panel_index: int32 [1], replicated, may hold values from 0 to 2
- prior_count: int32 [1], replicated, may hold values from 384 to 512
Outputs:
- new_basis: float32 [8192, 128], P(('rows', 'grp'))
- factors: float32 [640, 128], replicated
The draws below stay inside these ranges and needn't reach their ends.
All inputs are finite; a program needn't handle non-finite values.
Results may differ from the reference program's by a relative error of at most 0.00011.
Values sent between devices are 32-bit elements; how exact they have to be, the bound alone decides.
A program may use at most 64 MiB of HBM per device.

```python
import jax
import jax.numpy as jnp
from jax import lax

SK = 2048
NP = 512
P_SIZE = 64
BLOCK_PANELS = 4
ROWS = 8192


def draw_both(key):
    base = jax.random.fold_in(key, 11)
    first_key, second_key, third_key = jax.random.split(base, 3)
    place = jnp.arange(ROWS, dtype=jnp.float32) / max(ROWS - 1, 1)
    scales = 3.0 ** place
    basis = jax.random.normal(first_key, (ROWS, NP), jnp.float32)
    noise = jax.random.normal(third_key, (ROWS, BLOCK_PANELS * P_SIZE), jnp.float32)
    basis = basis * scales[:, None] * ROWS ** (-0.5)
    mixing = jax.random.normal(second_key, (NP, BLOCK_PANELS * P_SIZE), jnp.float32)
    panels = jnp.dot(basis, mixing) + 4.0 * ROWS ** (-0.5) * noise * scales[:, None]
    return (basis, panels)


def draw_prior_basis(key, part):
    return draw_both(key)[0]


def draw_panel_block(key, part):
    return draw_both(key)[1]


def steps_of(stream_key, dims, cuts, low, high):
    factor_of = 1.0
    for axis_at, parts in cuts:
        draws = jax.random.uniform(jax.random.fold_in(jax.random.fold_in(stream_key, 6), axis_at), (parts,), jnp.float32, low / len(cuts), high / len(cuts))
        factor_of = factor_of * jnp.repeat(jnp.exp(draws), dims[axis_at] // parts).reshape((-1,) + (1,) * (len(dims) - 1 - axis_at))
    return factor_of


def gaussian(key, dims, spread, reach, cuts=(), kind=jnp.bfloat16):
    loudness = steps_of(key, dims, cuts, -0.22, 0.18) if cuts else 1.0
    array = jax.random.normal(key, dims, jnp.float32) * spread * loudness
    return jnp.minimum(jnp.maximum(array, -reach), reach).astype(kind)


def setup_inputs(seed: int = 0) -> dict:
    splits = jax.random.split(jax.random.key(seed), 6)
    sketch = gaussian(splits[0], (SK, ROWS), SK ** -0.5, 0.125, ((1, 32),), jnp.float32)
    prior_basis = draw_prior_basis(jax.random.fold_in(splits[5], 71), 0)
    panel_block = draw_panel_block(jax.random.fold_in(splits[5], 71), 0)
    panel_index = jax.random.randint(splits[3], (1,), 0, BLOCK_PANELS - 1).astype(jnp.int32)
    prior_count = jax.random.randint(splits[4], (1,), NP - 2 * P_SIZE, NP + 1).astype(jnp.int32)
    return {"sketch": sketch, "prior_basis": prior_basis, "panel_block": panel_block, "panel_index": panel_index, "prior_count": prior_count}


def matmul(left, right):
    return jnp.dot(left, right, precision=lax.Precision.HIGHEST)

def right_solve(factor, values):
    return jax.scipy.linalg.solve_triangular(factor, values.T, lower=True).T

def reference(sketch, prior_basis, panel_block, panel_index, prior_count):
    width = prior_basis.shape[1]
    column_keep = (jnp.arange(width) < prior_count[0]).astype(jnp.float32)
    masked = prior_basis * column_keep
    start = (panel_index[0] * P_SIZE).astype(jnp.int32)
    chosen = lax.dynamic_slice_in_dim(panel_block, start, 2 * P_SIZE, 1)
    first = chosen[:, :P_SIZE]
    second = chosen[:, P_SIZE:]
    prior_sketch = matmul(sketch, masked)
    sketch_one = matmul(sketch, first)
    sketch_two = matmul(sketch, second)
    gram_prior = matmul(prior_sketch.T, prior_sketch) + jnp.diag(1.0 - column_keep)
    prior_factor = jnp.linalg.cholesky(gram_prior)
    coef_one = jax.scipy.linalg.cho_solve((prior_factor, True), matmul(prior_sketch.T, sketch_one))
    resid_one = first - matmul(masked, coef_one)
    skres_one = sketch_one - matmul(prior_sketch, coef_one)
    tri_one = jnp.linalg.cholesky(matmul(resid_one.T, resid_one))
    basis_one = right_solve(tri_one, resid_one)
    skbasis_one = right_solve(tri_one, skres_one)
    coef_two = jax.scipy.linalg.cho_solve((prior_factor, True), matmul(prior_sketch.T, sketch_two))
    resid_two = second - matmul(masked, coef_two)
    skres_two = sketch_two - matmul(prior_sketch, coef_two)
    small_factor = jnp.linalg.cholesky(matmul(skbasis_one.T, skbasis_one))
    inner = jax.scipy.linalg.cho_solve((small_factor, True), matmul(skbasis_one.T, skres_two))
    final_two = resid_two - matmul(basis_one, inner)
    tri_two = jnp.linalg.cholesky(matmul(final_two.T, final_two))
    basis_two = right_solve(tri_two, final_two)
    scale_rows = jnp.sqrt(jnp.float32(prior_basis.shape[0]))
    new_basis = jnp.concatenate([basis_one, basis_two], axis=1) * scale_rows
    upper = jnp.concatenate([tri_one.T, inner], axis=1)
    lower_rows = jnp.concatenate([jnp.zeros((P_SIZE, P_SIZE), jnp.float32), tri_two.T], axis=1)
    factors = jnp.concatenate([jnp.concatenate([coef_one, coef_two], axis=1), upper, lower_rows], axis=0)
    return (new_basis, factors)
```

```python
import functools

import jax
import jax.numpy as jnp
from jax import lax
from jax.experimental import pallas as pl
from jax.experimental.pallas import tpu as pltpu
from jax.sharding import PartitionSpec as P

P_SIZE = 64
T = 128
HIGHEST = lax.Precision.HIGHEST
F32 = jnp.float32
VMEM_LIMIT = 60 * 1024 * 1024


def dot(a, b, ca=1, cb=0):
    return lax.dot_general(
        a, b, (((ca,), (cb,)), ((), ())), precision=HIGHEST, preferred_element_type=F32
    )


def bits_of(size):
    out, b = [], 1
    while b < size:
        out.append(b)
        b *= 2
    return out


def orders(rows, grp):
    core = [("grp", b) for b in bits_of(grp)[:1]]
    y = [("grp", b) for b in bits_of(grp)[1:]]
    x = [("rows", b) for b in bits_of(rows)[:1]]
    z = [("rows", b) for b in bits_of(rows)[1:]]
    return core + x + y + z, core + y + x + z, core + z + x + y


def my_bit(axis, b):
    return (lax.axis_index(axis) // b) % 2


def peer(axis, b):
    me = lax.axis_index(axis)
    return {axis: me + b * (1 - 2 * my_bit(axis, b))}


def barrier_all(order):
    sem = pltpu.get_barrier_semaphore()
    for axis, b in order:
        pl.semaphore_signal(sem, inc=1, device_id=peer(axis, b), device_id_type=pl.DeviceIdType.MESH)
    pl.semaphore_wait(sem, len(order))


def remote(src, dst, send, recv, axis, b):
    return pltpu.make_async_remote_copy(
        src_ref=src, dst_ref=dst, send_sem=send, recv_sem=recv,
        device_id=peer(axis, b), device_id_type=pl.DeviceIdType.MESH,
    )


def block_at(order, target, n):
    k = len(order)
    spots = []
    for blk in range(n):
        value = {target[i]: (blk >> (k - 1 - i)) & 1 for i in range(k)}
        spots.append(sum(value[order[i]] << (k - 1 - i) for i in range(k)))
    return spots


def load_columns(idx_ref, cnt_ref, prior_ref, block_ref):
    width = prior_ref.shape[1]
    lane = lax.broadcasted_iota(jnp.int32, prior_ref.shape, 1)
    masked = jnp.where(lane < cnt_ref[0], prior_ref[...], 0.0)
    start = idx_ref[0]
    chosen = block_ref[:, 0:2 * P_SIZE]
    for s in range(1, block_ref.shape[1] // P_SIZE - 1):
        chosen = jnp.where(start == s, block_ref[:, s * P_SIZE:(s + 2) * P_SIZE], chosen)
    return masked, chosen


def reduce_scatter(parts, sems, base):
    k = len(parts[0][0])
    offs = [0] * len(parts)
    size = [acc.shape[0] for _, acc, _ in parts]
    pend = [None] * len(parts)
    send_sem, recv_sem = sems

    def start(q, i):
        order, acc, recvs = parts[q]
        axis, b = order[i]
        half = size[q] // 2
        bit = my_bit(axis, b)
        src = acc.at[pl.ds(pl.multiple_of(offs[q] + (1 - bit) * half, 8), half)]
        c = remote(src, recvs[i], send_sem.at[base + q, i], recv_sem.at[base + q, i], axis, b)
        c.start()
        offs[q] = offs[q] + bit * half
        size[q] = half
        pend[q] = c

    for q in range(len(parts)):
        start(q, 0)
    for i in range(k):
        for q in range(len(parts)):
            pend[q].wait()
            _, acc, recvs = parts[q]
            spot = pl.ds(pl.multiple_of(offs[q], 8), size[q])
            acc[spot] = acc[spot] + recvs[i][...]
            if i + 1 < k:
                start(q, i + 1)
    return offs, size


def gather(parts, offs, size, sems, base):
    k = len(parts[0][0])
    send_sem, recv_sem = sems
    offs, size = list(offs), list(size)
    pend = [None] * len(parts)

    def start(q, i):
        order, full = parts[q]
        axis, b = order[i]
        spot = pl.ds(pl.multiple_of(offs[q], 8), size[q])
        c = remote(full.at[spot], full.at[spot], send_sem.at[base + q, i], recv_sem.at[base + q, i], axis, b)
        c.start()
        offs[q] = offs[q] - my_bit(axis, b) * size[q]
        size[q] = size[q] * 2
        pend[q] = c

    for q in range(len(parts)):
        start(q, k - 1)
    for i in range(k - 1, -1, -1):
        for q in range(len(parts)):
            pend[q].wait()
            if i > 0:
                start(q, i - 1)


def gram_kernel(rows, grp, n_k, cols, grows, *refs):
    idx_ref, cnt_ref, sketch_ref, prior_ref, block_ref, full_a, full_b = refs[:7]
    rest = list(refs[7:])
    n = rows * grp
    ords = orders(rows, grp)
    accs = [rest.pop(0) for _ in cols]
    recvs = [[rest.pop(0) for _ in range(n_k)] for _ in cols]
    gaccs = [rest.pop(0) for _ in range(2)]
    grecvs = [[rest.pop(0) for _ in range(n_k)] for _ in range(2)]
    send_sem, recv_sem = rest
    sems = (send_sem, recv_sem)
    barrier_all(ords[0])
    masked, chosen = load_columns(idx_ref, cnt_ref, prior_ref, block_ref)
    right = jnp.concatenate([masked, chosen], axis=1)
    sk = sketch_ref.shape[0]
    per = sk // n
    step = 512
    for r in range(0, sk, step):
        prod = dot(sketch_ref[r:r + step, :], right)
        lane = 0
        for q, w in enumerate(cols):
            spots = block_at(ords[q], ords[0], n)
            if q == 0:
                accs[q][r:r + step, :] = prod[:, lane:lane + w]
            else:
                for blk in range(r // per, (r + step) // per):
                    s = spots[blk] * per
                    accs[q][s:s + per, :] = prod[blk * per - r:(blk + 1) * per - r, lane:lane + w]
            lane += w
    offs, size = reduce_scatter(
        [(ords[q], accs[q], recvs[q]) for q in range(len(cols))], sems, 0
    )
    mine = jnp.concatenate(
        [accs[q][pl.ds(pl.multiple_of(offs[q], 8), per)] for q in range(len(cols))], axis=1
    )
    gram = dot(mine, mine, 0, 0)
    width = gram.shape[0] // T
    t = 0
    per_part = 8
    for i in range(width):
        for j in range(i + 1):
            q, s = t // per_part, (t % per_part) * T
            gaccs[q][s:s + T, :] = gram[i * T:(i + 1) * T, j * T:(j + 1) * T]
            t += 1
    for q in range(2):
        used = min(per_part, t - q * per_part) * T
        if used < grows:
            gaccs[q][used:grows, :] = jnp.zeros((grows - used, T), F32)
    parts = [(ords[q], gaccs[q], grecvs[q]) for q in range(2)]
    offs, size = reduce_scatter(parts, sems, len(cols))
    for q, full in enumerate((full_a, full_b)):
        spot = pl.ds(pl.multiple_of(offs[q], 8), size[q])
        full[spot] = gaccs[q][spot]
    gather([(ords[0], full_a), (ords[1], full_b)], offs, size, sems, len(cols) + 2)


def solve_kernel(idx_ref, cnt_ref, prior_ref, block_ref, ta_ref, tb_ref,
                 coef_ref, x_ref, resid_ref, gram_ref, a_ref, inv_ref):
    width = prior_ref.shape[1]
    blocks = width // T + 1
    t = 0
    for i in range(blocks):
        for j in range(i + 1):
            src, s = (ta_ref, t * T) if t < 8 else (tb_ref, (t - 8) * T)
            tile = src[s:s + T, :]
            if i == j and i < blocks - 1:
                row = lax.broadcasted_iota(jnp.int32, (T, T), 0)
                col = lax.broadcasted_iota(jnp.int32, (T, T), 1)
                tile = tile + jnp.where((row == col) & (row + i * T >= cnt_ref[0]), 1.0, 0.0)
            a_ref[i * T:(i + 1) * T, j * T:(j + 1) * T] = tile
            if i != j:
                a_ref[j * T:(j + 1) * T, i * T:(i + 1) * T] = tile.T
            t += 1

    lane = lax.broadcasted_iota(jnp.int32, (T, T), 1)
    sub = lax.broadcasted_iota(jnp.int32, (8, T), 0)
    lane8 = lax.broadcasted_iota(jnp.int32, (1, T), 1)

    def body(k, _):
        at = pl.ds(pl.multiple_of(k * T, T), T)
        d = a_ref[at, at]
        tiles = [d[8 * v:8 * v + 8, :] for v in range(T // 8)]
        for p in range(T):
            v, o = p // 8, p % 8
            row = tiles[v][o:o + 1, :]
            piv = 1.0 / row[:, p:p + 1]
            row = jnp.where(lane8 == p, piv, row * piv)
            new = []
            for u in range(T // 8):
                col = tiles[u][:, p:p + 1]
                base = jnp.where(lane8 == p, 0.0, tiles[u])
                w = base - col * row
                if u == v:
                    w = jnp.where(sub == o, row, w)
                new.append(w)
            tiles = new
        inv = jnp.concatenate(tiles, axis=0)
        rowk = dot(inv, a_ref[at, :])
        colk = a_ref[:, at]
        a_ref[...] = a_ref[...] - dot(colk, rowk)
        a_ref[at, :] = rowk
        return 0

    lax.fori_loop(0, blocks - 1, body, 0)
    coef = a_ref[0:width, width:width + T]
    coef_ref[...] = coef
    e = a_ref[width:width + P_SIZE, width:width + T]
    tiles = [e[8 * v:8 * v + 8, :] for v in range(P_SIZE // 8)]
    for p in range(P_SIZE):
        v, o = p // 8, p % 8
        row = tiles[v][o:o + 1, :]
        row = row / row[:, p:p + 1]
        new = []
        for u in range(P_SIZE // 8):
            w = tiles[u] - tiles[u][:, p:p + 1] * row
            if u == v:
                w = jnp.where(sub == o, row, w)
            new.append(w)
        tiles = new
    x = jnp.concatenate(tiles, axis=0)[:, P_SIZE:]
    x_ref[...] = x
    masked, chosen = load_columns(idx_ref, cnt_ref, prior_ref, block_ref)
    resid = chosen - dot(masked, coef)
    one = resid[:, :P_SIZE]
    two = resid[:, P_SIZE:] - dot(one, x)
    resid_ref[...] = jnp.concatenate([one, two], axis=1)
    gram_ref[...] = jnp.concatenate([dot(one, one, 0, 0), dot(two, two, 0, 0)], axis=1)


def finish_kernel(order, scale, gram_ref, resid_ref, x_ref, coef_ref, basis_ref, factors_ref,
                  hold, recv, send_sem, recv_sem):
    barrier_all(order)
    k = len(order)
    for i, (axis, b) in enumerate(order):
        src = gram_ref if i == 0 else hold.at[i - 1]
        c = remote(src, recv.at[i], send_sem.at[i], recv_sem.at[i], axis, b)
        c.start()
        c.wait()
        hold[i] = src[...] + recv[i]
    gram = hold[k - 1]
    eye = (lax.broadcasted_iota(jnp.int32, (P_SIZE, P_SIZE), 0)
           == lax.broadcasted_iota(jnp.int32, (P_SIZE, P_SIZE), 1)).astype(F32)
    sub = lax.broadcasted_iota(jnp.int32, (8, T), 0)
    mats = []
    for h in range(2):
        m = jnp.concatenate([gram[:, h * P_SIZE:(h + 1) * P_SIZE], eye], axis=1)
        mats.append([m[8 * v:8 * v + 8, :] for v in range(P_SIZE // 8)])
    for p in range(P_SIZE):
        v, o = p // 8, p % 8
        for h in range(2):
            tiles = mats[h]
            row = tiles[v][o:o + 1, :]
            d = row[:, p:p + 1]
            y = lax.rsqrt(d)
            y = y * (1.5 - 0.5 * d * y * y)
            row = row * y
            new = list(tiles)
            for u in range(v, P_SIZE // 8):
                w = tiles[u] - (tiles[u][:, p:p + 1] * y) * row
                if u == v:
                    w = jnp.where(sub == o, row, jnp.where(sub > o, w, tiles[u]))
                new[u] = w
            mats[h] = new
    full = [jnp.concatenate(m, axis=0) for m in mats]
    row = lax.broadcasted_iota(jnp.int32, (P_SIZE, P_SIZE), 0)
    col = lax.broadcasted_iota(jnp.int32, (P_SIZE, P_SIZE), 1)
    upper = [jnp.where(row <= col, f[:, :P_SIZE], 0.0) for f in full]
    lowinv = [f[:, P_SIZE:] for f in full]
    basis_ref[...] = jnp.concatenate(
        [dot(resid_ref[:, h * P_SIZE:(h + 1) * P_SIZE], lowinv[h], 1, 1) for h in range(2)], axis=1
    ) * scale
    width = coef_ref.shape[0]
    factors_ref[0:width, :] = coef_ref[...]
    inner = dot(upper[0], x_ref[...])
    factors_ref[width:width + P_SIZE, :] = jnp.concatenate([upper[0], inner], axis=1)
    factors_ref[width + P_SIZE:, :] = jnp.concatenate([jnp.zeros_like(eye), upper[1]], axis=1)


def shards(rows, grp, sketch, prior, block, idx, cnt):
    n = rows * grp
    n_k = len(orders(rows, grp)[0])
    sk, local = sketch.shape
    width = prior.shape[1]
    vm = pl.BlockSpec(memory_space=pltpu.VMEM)
    sm = pl.BlockSpec(memory_space=pltpu.SMEM)
    cols = (2 * T, 2 * T, width + T - 4 * T)
    grows = n * max(8, 8 * T // n)
    scratch = [pltpu.VMEM((sk, w), F32) for w in cols]
    for w in cols:
        scratch += [pltpu.VMEM((sk >> (i + 1), w), F32) for i in range(n_k)]
    scratch += [pltpu.VMEM((grows, T), F32)] * 2
    for _ in range(2):
        scratch += [pltpu.VMEM((grows >> (i + 1), T), F32) for i in range(n_k)]
    scratch += [pltpu.SemaphoreType.DMA((7, n_k))] * 2
    tiles = pl.pallas_call(
        functools.partial(gram_kernel, rows, grp, n_k, cols, grows),
        out_shape=[jax.ShapeDtypeStruct((grows, T), F32)] * 2,
        in_specs=[sm, sm, vm, vm, vm],
        out_specs=[vm, vm],
        scratch_shapes=scratch,
        compiler_params=pltpu.CompilerParams(
            collective_id=0, has_side_effects=True, vmem_limit_bytes=VMEM_LIMIT
        ),
    )(idx, cnt, sketch, prior, block)
    coef, x, resid, gram = pl.pallas_call(
        solve_kernel,
        out_shape=[
            jax.ShapeDtypeStruct((width, T), F32),
            jax.ShapeDtypeStruct((P_SIZE, P_SIZE), F32),
            jax.ShapeDtypeStruct((local, T), F32),
            jax.ShapeDtypeStruct((P_SIZE, T), F32),
        ],
        in_specs=[sm, sm, vm, vm, vm, vm],
        out_specs=[vm] * 4,
        scratch_shapes=[pltpu.VMEM((width + T, width + T), F32), pltpu.VMEM((T, T), F32)],
        compiler_params=pltpu.CompilerParams(vmem_limit_bytes=VMEM_LIMIT),
    )(idx, cnt, prior, block, *tiles)
    order = orders(rows, grp)[0]
    scale = float(local * n) ** 0.5
    return tuple(pl.pallas_call(
        functools.partial(finish_kernel, order, scale),
        out_shape=[
            jax.ShapeDtypeStruct((local, T), F32),
            jax.ShapeDtypeStruct((width + T, T), F32),
        ],
        in_specs=[vm] * 4,
        out_specs=[vm] * 2,
        scratch_shapes=[
            pltpu.VMEM((n_k, P_SIZE, T), F32),
            pltpu.VMEM((n_k, P_SIZE, T), F32),
            pltpu.SemaphoreType.DMA((n_k,)),
            pltpu.SemaphoreType.DMA((n_k,)),
        ],
        compiler_params=pltpu.CompilerParams(
            collective_id=1, has_side_effects=True, vmem_limit_bytes=VMEM_LIMIT
        ),
    )(gram, resid, x, coef))


def solution(mesh):
    rows, grp = mesh.shape["rows"], mesh.shape["grp"]
    placed = (
        P(None, ("rows", "grp")),
        P(("rows", "grp"), None),
        P(("rows", "grp"), None),
        P(),
        P(),
    )
    return jax.shard_map(
        functools.partial(shards, rows, grp),
        mesh=mesh,
        in_specs=placed,
        out_specs=(P(("rows", "grp"), None), P()),
        check_vma=False,
    )
```

```python
import functools

import jax
import jax.numpy as jnp
from jax import lax
from jax.experimental import pallas as pl
from jax.experimental.pallas import tpu as pltpu
from jax.sharding import PartitionSpec as P

P_SIZE = 64
T = 128
HIGHEST = lax.Precision.HIGHEST
F32 = jnp.float32
VMEM_LIMIT = 60 * 1024 * 1024


def dot(a, b, ca=1, cb=0):
    return lax.dot_general(
        a, b, (((ca,), (cb,)), ((), ())), precision=HIGHEST, preferred_element_type=F32
    )


def split(x):
    hi = x.astype(jnp.bfloat16)
    return hi, (x - hi.astype(F32)).astype(jnp.bfloat16)


def dot3(a, b):
    ah, al = a
    bh, bl = b
    out = jnp.dot(ah, bl, preferred_element_type=F32)
    out = out + jnp.dot(al, bh, preferred_element_type=F32)
    return out + jnp.dot(ah, bh, preferred_element_type=F32)


def bits_of(size):
    out, b = [], 1
    while b < size:
        out.append(b)
        b *= 2
    return out


def orders(rows, grp):
    core = [("grp", b) for b in bits_of(grp)[:1]]
    y = [("grp", b) for b in bits_of(grp)[1:]]
    x = [("rows", b) for b in bits_of(rows)[:1]]
    z = [("rows", b) for b in bits_of(rows)[1:]]
    return core + x + y + z, core + y + x + z, core + z + x + y


def my_bit(axis, b):
    return (lax.axis_index(axis) // b) % 2


def peer(axis, b):
    me = lax.axis_index(axis)
    return {axis: me + b * (1 - 2 * my_bit(axis, b))}


def barrier_all(order):
    sem = pltpu.get_barrier_semaphore()
    for axis, b in order:
        pl.semaphore_signal(sem, inc=1, device_id=peer(axis, b), device_id_type=pl.DeviceIdType.MESH)
    pl.semaphore_wait(sem, len(order))


def remote(src, dst, send, recv, axis, b):
    return pltpu.make_async_remote_copy(
        src_ref=src, dst_ref=dst, send_sem=send, recv_sem=recv,
        device_id=peer(axis, b), device_id_type=pl.DeviceIdType.MESH,
    )


def block_at(order, target, n):
    k = len(order)
    spots = []
    for blk in range(n):
        value = {target[i]: (blk >> (k - 1 - i)) & 1 for i in range(k)}
        spots.append(sum(value[order[i]] << (k - 1 - i) for i in range(k)))
    return spots


def load_columns(idx_ref, cnt_ref, prior_ref, block_ref):
    width = prior_ref.shape[1]
    lane = lax.broadcasted_iota(jnp.int32, prior_ref.shape, 1)
    masked = jnp.where(lane < cnt_ref[0], prior_ref[...], 0.0)
    start = idx_ref[0]
    chosen = block_ref[:, 0:2 * P_SIZE]
    for s in range(1, block_ref.shape[1] // P_SIZE - 1):
        chosen = jnp.where(start == s, block_ref[:, s * P_SIZE:(s + 2) * P_SIZE], chosen)
    return masked, chosen


def reduce_scatter(parts, sems, base):
    k = len(parts[0][0])
    offs = [0] * len(parts)
    size = [acc.shape[0] for _, acc, _ in parts]
    pend = [None] * len(parts)
    send_sem, recv_sem = sems

    def start(q, i):
        order, acc, recvs = parts[q]
        axis, b = order[i]
        half = size[q] // 2
        bit = my_bit(axis, b)
        src = acc.at[pl.ds(pl.multiple_of(offs[q] + (1 - bit) * half, 8), half)]
        c = remote(src, recvs[i], send_sem.at[base + q, i], recv_sem.at[base + q, i], axis, b)
        c.start()
        offs[q] = offs[q] + bit * half
        size[q] = half
        pend[q] = c

    for q in range(len(parts)):
        start(q, 0)
    for i in range(k):
        for q in range(len(parts)):
            pend[q].wait()
            _, acc, recvs = parts[q]
            spot = pl.ds(pl.multiple_of(offs[q], 8), size[q])
            acc[spot] = acc[spot] + recvs[i][...]
            if i + 1 < k:
                start(q, i + 1)
    return offs, size


def gather(parts, offs, size, sems, base):
    k = len(parts[0][0])
    send_sem, recv_sem = sems
    offs, size = list(offs), list(size)
    pend = [None] * len(parts)

    def start(q, i):
        order, full = parts[q]
        axis, b = order[i]
        spot = pl.ds(pl.multiple_of(offs[q], 8), size[q])
        c = remote(full.at[spot], full.at[spot], send_sem.at[base + q, i], recv_sem.at[base + q, i], axis, b)
        c.start()
        offs[q] = offs[q] - my_bit(axis, b) * size[q]
        size[q] = size[q] * 2
        pend[q] = c

    for q in range(len(parts)):
        start(q, k - 1)
    for i in range(k - 1, -1, -1):
        for q in range(len(parts)):
            pend[q].wait()
            if i > 0:
                start(q, i - 1)


def gram_kernel(rows, grp, n_k, cols, grows, *refs):
    idx_ref, cnt_ref, sketch_ref, prior_ref, block_ref, full_a, full_b = refs[:7]
    rest = list(refs[7:])
    n = rows * grp
    ords = orders(rows, grp)
    accs = [rest.pop(0) for _ in cols]
    recvs = [[rest.pop(0) for _ in range(n_k)] for _ in cols]
    gaccs = [rest.pop(0) for _ in range(2)]
    grecvs = [[rest.pop(0) for _ in range(n_k)] for _ in range(2)]
    send_sem, recv_sem = rest
    sems = (send_sem, recv_sem)
    barrier_all(ords[0])
    masked, chosen = load_columns(idx_ref, cnt_ref, prior_ref, block_ref)
    right = split(jnp.concatenate([masked, chosen], axis=1))
    sk = sketch_ref.shape[0]
    per = sk // n
    step = 512
    for r in range(0, sk, step):
        prod = dot3(split(sketch_ref[r:r + step, :]), right)
        lane = 0
        for q, w in enumerate(cols):
            spots = block_at(ords[q], ords[0], n)
            if q == 0:
                accs[q][r:r + step, :] = prod[:, lane:lane + w]
            else:
                for blk in range(r // per, (r + step) // per):
                    s = spots[blk] * per
                    accs[q][s:s + per, :] = prod[blk * per - r:(blk + 1) * per - r, lane:lane + w]
            lane += w
    offs, size = reduce_scatter(
        [(ords[q], accs[q], recvs[q]) for q in range(len(cols))], sems, 0
    )
    mine = jnp.concatenate(
        [accs[q][pl.ds(pl.multiple_of(offs[q], 8), per)] for q in range(len(cols))], axis=1
    )
    gram = dot(mine, mine, 0, 0)
    width = gram.shape[0] // T
    t = 0
    per_part = 8
    for i in range(width):
        for j in range(i + 1):
            q, s = t // per_part, (t % per_part) * T
            gaccs[q][s:s + T, :] = gram[i * T:(i + 1) * T, j * T:(j + 1) * T]
            t += 1
    for q in range(2):
        used = min(per_part, t - q * per_part) * T
        if used < grows:
            gaccs[q][used:grows, :] = jnp.zeros((grows - used, T), F32)
    parts = [(ords[q], gaccs[q], grecvs[q]) for q in range(2)]
    offs, size = reduce_scatter(parts, sems, len(cols))
    for q, full in enumerate((full_a, full_b)):
        spot = pl.ds(pl.multiple_of(offs[q], 8), size[q])
        full[spot] = gaccs[q][spot]
    gather([(ords[0], full_a), (ords[1], full_b)], offs, size, sems, len(cols) + 2)


def sweep4(tiles, p, inverse):
    v, o = p // 8, p % 8
    lane = lax.broadcasted_iota(jnp.int32, (8, T), 1)
    sub = lax.broadcasted_iota(jnp.int32, (8, T), 0)
    r = [jnp.broadcast_to(tiles[v][o + i:o + i + 1, :], (8, T)) for i in range(4)]

    def at(i, j):
        return jnp.broadcast_to(r[i][:, p + j:p + j + 1], (8, T))

    a, b, e, f = at(0, 0), at(0, 1), at(0, 2), at(0, 3)
    c, g, h = at(1, 1), at(1, 2), at(1, 3)
    x, y, z = at(2, 2), at(2, 3), at(3, 3)
    ra = 1.0 / (a * c - b * b)
    k00, k01 = (c * e - b * g) * ra, (c * f - b * h) * ra
    k10, k11 = (a * g - b * e) * ra, (a * h - b * f) * ra
    s00 = x - (e * k00 + g * k10)
    s01 = y - (e * k01 + g * k11)
    s11 = z - (f * k01 + h * k11)
    rs = 1.0 / (s00 * s11 - s01 * s01)
    inside = (lane >= p) & (lane < p + 4)
    if inverse:
        r = [jnp.where(inside, jnp.where(lane == p + i, 1.0, 0.0), r[i]) for i in range(4)]
    g0, g1 = (c * r[0] - b * r[1]) * ra, (a * r[1] - b * r[0]) * ra
    q2 = r[2] - (k00 * r[0] + k10 * r[1])
    q3 = r[3] - (k01 * r[0] + k11 * r[1])
    n2, n3 = (s11 * q2 - s01 * q3) * rs, (s00 * q3 - s01 * q2) * rs
    n0, n1 = g0 - (k00 * n2 + k01 * n3), g1 - (k10 * n2 + k11 * n3)
    new = []
    for u, tile in enumerate(tiles):
        w = jnp.where(inside, 0.0, tile) if inverse else tile
        for j, row in enumerate((n0, n1, n2, n3)):
            w = w - tile[:, p + j:p + j + 1] * row
        if u == v:
            for j, row in enumerate((n0, n1, n2, n3)):
                w = jnp.where(sub == o + j, row, w)
        new.append(w)
    return new


def solve_kernel(idx_ref, cnt_ref, prior_ref, block_ref, ta_ref, tb_ref,
                 coef_ref, x_ref, resid_ref, gram_ref, a_ref, inv_ref):
    width = prior_ref.shape[1]
    blocks = width // T + 1
    t = 0
    for i in range(blocks):
        for j in range(i + 1):
            src, s = (ta_ref, t * T) if t < 8 else (tb_ref, (t - 8) * T)
            tile = src[s:s + T, :]
            if i == j and i < blocks - 1:
                row = lax.broadcasted_iota(jnp.int32, (T, T), 0)
                col = lax.broadcasted_iota(jnp.int32, (T, T), 1)
                tile = tile + jnp.where((row == col) & (row + i * T >= cnt_ref[0]), 1.0, 0.0)
            a_ref[i * T:(i + 1) * T, j * T:(j + 1) * T] = tile
            if i != j:
                a_ref[j * T:(j + 1) * T, i * T:(i + 1) * T] = tile.T
            t += 1

    def body(k, _):
        at = pl.ds(pl.multiple_of(k * T, T), T)
        d = a_ref[at, at]
        tiles = [d[8 * v:8 * v + 8, :] for v in range(T // 8)]
        for p in range(0, T, 4):
            tiles = sweep4(tiles, p, True)
        inv_ref[...] = jnp.concatenate(tiles, axis=0)
        for kk in range(blocks - 1):
            @pl.when(k == kk)
            def _():
                own, rest = slice(kk * T, (kk + 1) * T), slice((kk + 1) * T, blocks * T)
                rowk = dot(inv_ref[...], a_ref[own, rest])
                if kk:
                    top = slice(0, kk * T)
                    a_ref[top, rest] = a_ref[top, rest] - dot(a_ref[top, own], rowk)
                a_ref[rest, rest] = a_ref[rest, rest] - dot(a_ref[rest, own], rowk)
                a_ref[own, rest] = rowk
        return 0

    lax.fori_loop(0, blocks - 1, body, 0)
    coef = a_ref[0:width, width:width + T]
    coef_ref[...] = coef
    e = a_ref[width:width + P_SIZE, width:width + T]
    tiles = [e[8 * v:8 * v + 8, :] for v in range(P_SIZE // 8)]
    for p in range(0, P_SIZE, 4):
        tiles = sweep4(tiles, p, False)
    x = jnp.concatenate(tiles, axis=0)[:, P_SIZE:]
    x_ref[...] = x
    masked, chosen = load_columns(idx_ref, cnt_ref, prior_ref, block_ref)
    resid = chosen - dot(masked, coef)
    one = resid[:, :P_SIZE]
    two = resid[:, P_SIZE:] - dot(one, x)
    resid_ref[...] = jnp.concatenate([one, two], axis=1)
    gram_ref[...] = jnp.concatenate([dot(one, one, 0, 0), dot(two, two, 0, 0)], axis=1)


def sum_kernel(order, gram_ref, out_ref, hold, recv, send_sem, recv_sem):
    barrier_all(order)
    k = len(order)
    for i, (axis, b) in enumerate(order):
        src = gram_ref if i == 0 else hold.at[i - 1]
        c = remote(src, recv.at[i], send_sem.at[i], recv_sem.at[i], axis, b)
        c.start()
        c.wait()
        dst = out_ref if i == k - 1 else hold.at[i]
        dst[...] = src[...] + recv[i]


def finish_kernel(scale, gram_ref, resid_ref, x_ref, coef_ref, basis_ref, factors_ref):
    gram = gram_ref[...]
    eye = (lax.broadcasted_iota(jnp.int32, (P_SIZE, P_SIZE), 0)
           == lax.broadcasted_iota(jnp.int32, (P_SIZE, P_SIZE), 1)).astype(F32)
    sub = lax.broadcasted_iota(jnp.int32, (8, T), 0)
    mats = []
    for h in range(2):
        m = jnp.concatenate([gram[:, h * P_SIZE:(h + 1) * P_SIZE], eye], axis=1)
        mats.append([m[8 * v:8 * v + 8, :] for v in range(P_SIZE // 8)])
    for p in range(P_SIZE):
        v, o = p // 8, p % 8
        for h in range(2):
            tiles = mats[h]
            row = tiles[v][o:o + 1, :]
            d = row[:, p:p + 1]
            y = lax.rsqrt(d)
            y = y * (1.5 - 0.5 * d * y * y)
            row = row * y
            new = list(tiles)
            for u in range(v, P_SIZE // 8):
                w = tiles[u] - (tiles[u][:, p:p + 1] * y) * row
                if u == v:
                    w = jnp.where(sub == o, row, jnp.where(sub > o, w, tiles[u]))
                new[u] = w
            mats[h] = new
    full = [jnp.concatenate(m, axis=0) for m in mats]
    row = lax.broadcasted_iota(jnp.int32, (P_SIZE, P_SIZE), 0)
    col = lax.broadcasted_iota(jnp.int32, (P_SIZE, P_SIZE), 1)
    upper = [jnp.where(row <= col, f[:, :P_SIZE], 0.0) for f in full]
    lowinv = [f[:, P_SIZE:] for f in full]
    basis_ref[...] = jnp.concatenate(
        [dot(resid_ref[:, h * P_SIZE:(h + 1) * P_SIZE], lowinv[h], 1, 1) for h in range(2)], axis=1
    ) * scale
    width = coef_ref.shape[0]
    factors_ref[0:width, :] = coef_ref[...]
    inner = dot(upper[0], x_ref[...])
    factors_ref[width:width + P_SIZE, :] = jnp.concatenate([upper[0], inner], axis=1)
    factors_ref[width + P_SIZE:, :] = jnp.concatenate([jnp.zeros_like(eye), upper[1]], axis=1)


def shards(rows, grp, sketch, prior, block, idx, cnt):
    n = rows * grp
    n_k = len(orders(rows, grp)[0])
    sk, local = sketch.shape
    width = prior.shape[1]
    vm = pl.BlockSpec(memory_space=pltpu.VMEM)
    sm = pl.BlockSpec(memory_space=pltpu.SMEM)
    cols = (2 * T, 2 * T, width + T - 4 * T)
    grows = n * max(8, 8 * T // n)
    scratch = [pltpu.VMEM((sk, w), F32) for w in cols]
    for w in cols:
        scratch += [pltpu.VMEM((sk >> (i + 1), w), F32) for i in range(n_k)]
    scratch += [pltpu.VMEM((grows, T), F32)] * 2
    for _ in range(2):
        scratch += [pltpu.VMEM((grows >> (i + 1), T), F32) for i in range(n_k)]
    scratch += [pltpu.SemaphoreType.DMA((7, n_k))] * 2
    tiles = pl.pallas_call(
        functools.partial(gram_kernel, rows, grp, n_k, cols, grows),
        out_shape=[jax.ShapeDtypeStruct((grows, T), F32)] * 2,
        in_specs=[sm, sm, vm, vm, vm],
        out_specs=[vm, vm],
        scratch_shapes=scratch,
        compiler_params=pltpu.CompilerParams(
            collective_id=0, has_side_effects=True, vmem_limit_bytes=VMEM_LIMIT
        ),
    )(idx, cnt, sketch, prior, block)
    coef, x, resid, gram = pl.pallas_call(
        solve_kernel,
        out_shape=[
            jax.ShapeDtypeStruct((width, T), F32),
            jax.ShapeDtypeStruct((P_SIZE, P_SIZE), F32),
            jax.ShapeDtypeStruct((local, T), F32),
            jax.ShapeDtypeStruct((P_SIZE, T), F32),
        ],
        in_specs=[sm, sm, vm, vm, vm, vm],
        out_specs=[vm] * 4,
        scratch_shapes=[pltpu.VMEM((width + T, width + T), F32), pltpu.VMEM((T, T), F32)],
        compiler_params=pltpu.CompilerParams(vmem_limit_bytes=VMEM_LIMIT),
    )(idx, cnt, prior, block, *tiles)
    order = orders(rows, grp)[0]
    scale = float(local * n) ** 0.5
    gram = pl.pallas_call(
        functools.partial(sum_kernel, order),
        out_shape=jax.ShapeDtypeStruct((P_SIZE, T), F32),
        in_specs=[vm],
        out_specs=vm,
        scratch_shapes=[
            pltpu.VMEM((n_k, P_SIZE, T), F32),
            pltpu.VMEM((n_k, P_SIZE, T), F32),
            pltpu.SemaphoreType.DMA((n_k,)),
            pltpu.SemaphoreType.DMA((n_k,)),
        ],
        compiler_params=pltpu.CompilerParams(collective_id=1, has_side_effects=True),
    )(gram)
    return tuple(pl.pallas_call(
        functools.partial(finish_kernel, scale),
        out_shape=[
            jax.ShapeDtypeStruct((local, T), F32),
            jax.ShapeDtypeStruct((width + T, T), F32),
        ],
        in_specs=[vm] * 4,
        out_specs=[vm] * 2,
        compiler_params=pltpu.CompilerParams(vmem_limit_bytes=VMEM_LIMIT),
    )(gram, resid, x, coef))


def solution(mesh):
    rows, grp = mesh.shape["rows"], mesh.shape["grp"]
    placed = (
        P(None, ("rows", "grp")),
        P(("rows", "grp"), None),
        P(("rows", "grp"), None),
        P(),
        P(),
    )
    return jax.shard_map(
        functools.partial(shards, rows, grp),
        mesh=mesh,
        in_specs=placed,
        out_specs=(P(("rows", "grp"), None), P()),
        check_vma=False,
    )
```

```python
import functools

import jax
import jax.numpy as jnp
from jax import lax
from jax.experimental import pallas as pl
from jax.experimental.pallas import tpu as pltpu
from jax.sharding import PartitionSpec as P

P_SIZE = 64
T = 128
HIGHEST = lax.Precision.HIGHEST
F32 = jnp.float32
VMEM_LIMIT = 60 * 1024 * 1024


def dot(a, b, ca=1, cb=0):
    return lax.dot_general(
        a, b, (((ca,), (cb,)), ((), ())), precision=HIGHEST, preferred_element_type=F32
    )


def split(x):
    hi = x.astype(jnp.bfloat16)
    return hi, (x - hi.astype(F32)).astype(jnp.bfloat16)


def dot3(a, b):
    ah, al = a
    bh, bl = b
    out = jnp.dot(ah, bl, preferred_element_type=F32)
    out = out + jnp.dot(al, bh, preferred_element_type=F32)
    return out + jnp.dot(ah, bh, preferred_element_type=F32)


def bits_of(size):
    out, b = [], 1
    while b < size:
        out.append(b)
        b *= 2
    return out


def axes_of(rows, grp):
    core = [("grp", b) for b in bits_of(grp)[:1]]
    y = [("grp", b) for b in bits_of(grp)[1:]]
    x = [("rows", b) for b in bits_of(rows)[:1]]
    z = [("rows", b) for b in bits_of(rows)[1:]]
    return core, y, x, z


def my_bit(axis, b):
    return (lax.axis_index(axis) // b) % 2


def peer(group, pattern):
    out = {}
    for i, (axis, b) in enumerate(group):
        if (pattern >> (len(group) - 1 - i)) & 1:
            here = out.get(axis, lax.axis_index(axis))
            out[axis] = here + b * (1 - 2 * my_bit(axis, b))
    return out


def spot_in(group, pattern=0):
    k, at = len(group), 0
    for i, (axis, b) in enumerate(group):
        flip, bit = (pattern >> (k - 1 - i)) & 1, my_bit(axis, b)
        at = at + (1 - bit if flip else bit) * (1 << (k - 1 - i))
    return at


def barrier_all(groups):
    sem = pltpu.get_barrier_semaphore()
    count = 0
    for group in groups:
        for pattern in range(1, 1 << len(group)):
            pl.semaphore_signal(
                sem, inc=1, device_id=peer(group, pattern), device_id_type=pl.DeviceIdType.MESH
            )
            count += 1
    pl.semaphore_wait(sem, count)


def remote(src, dst, send, recv, group, pattern):
    return pltpu.make_async_remote_copy(
        src_ref=src, dst_ref=dst, send_sem=send, recv_sem=recv,
        device_id=peer(group, pattern), device_id_type=pl.DeviceIdType.MESH,
    )


def rows_at(start, size):
    return pl.ds(pl.multiple_of(start, 8), size)


class Halving:
    def __init__(self, stages, acc, recvs, sends, arrives, full=None, gsends=None, garrives=None):
        self.stages, self.acc, self.recvs, self.full = stages, acc, recvs, full
        self.sems, self.gsems = (sends, arrives), (gsends, garrives)
        self.off, self.size, self.pend = 0, acc.shape[0], []

    def start(self, i):
        group = self.stages[i]
        sub = self.size >> len(group)
        self.pend = []
        for m in range(1, 1 << len(group)):
            src = self.acc.at[rows_at(self.off + spot_in(group, m) * sub, sub)]
            c = remote(src, self.recvs[i].at[m - 1], self.sems[0].at[i, m - 1],
                       self.sems[1].at[i, m - 1], group, m)
            c.start()
            self.pend.append(c)
        self.off = self.off + spot_in(group) * sub
        self.size = sub

    def finish(self, i):
        for c in self.pend:
            c.wait()
        at = rows_at(self.off, self.size)
        total = self.acc[at]
        for m in range(len(self.pend)):
            total = total + self.recvs[i][m]
        self.acc[at] = total

    def gstart(self, i):
        group = self.stages[i]
        self.pend = []
        at = self.full.at[rows_at(self.off, self.size)]
        for m in range(1, 1 << len(group)):
            c = remote(at, at, self.gsems[0].at[i, m - 1], self.gsems[1].at[i, m - 1], group, m)
            c.start()
            self.pend.append(c)
        self.off = self.off - spot_in(group) * self.size
        self.size = self.size << len(group)

    def gfinish(self):
        for c in self.pend:
            c.wait()


def recv_shapes(stages, rows, lanes):
    out = []
    for group in stages:
        rows = rows >> len(group)
        out.append(pltpu.VMEM(((1 << len(group)) - 1, rows, lanes), F32))
    return out


def sem_shape(stages):
    return pltpu.SemaphoreType.DMA((len(stages), max((1 << len(g)) - 1 for g in stages)))


def sketch_plan(rows, grp):
    core, y, x, z = axes_of(rows, grp)
    one = lambda bits: [[b] for b in bits]
    first, second, third = one(core + x + y + z), one(core + y + x + z), one(core + z + x + y)
    return [first, second, third, first, second]


def gram_plan(rows, grp):
    core, y, x, z = axes_of(rows, grp)
    return [[g for g in (core, x + y, z) if g], [g for g in (core, z, x + y) if g]]


def block_at(order, target, n):
    k = len(order)
    spots = []
    for blk in range(n):
        value = {target[i]: (blk >> (k - 1 - i)) & 1 for i in range(k)}
        spots.append(sum(value[order[i]] << (k - 1 - i) for i in range(k)))
    return spots


def load_columns(idx_ref, cnt_ref, prior_ref, block_ref):
    width = prior_ref.shape[1]
    lane = lax.broadcasted_iota(jnp.int32, prior_ref.shape, 1)
    masked = jnp.where(lane < cnt_ref[0], prior_ref[...], 0.0)
    start = idx_ref[0]
    chosen = block_ref[:, 0:2 * P_SIZE]
    for s in range(1, block_ref.shape[1] // P_SIZE - 1):
        chosen = jnp.where(start == s, block_ref[:, s * P_SIZE:(s + 2) * P_SIZE], chosen)
    return masked, chosen


def gram_kernel(rows, grp, grows, idx_ref, cnt_ref, sketch_ref, prior_ref, block_ref,
                full_a, full_b, *rest):
    rest = list(rest)
    n = rows * grp
    high, low = rest.pop(0), rest.pop(0)
    plan, gplan = sketch_plan(rows, grp), gram_plan(rows, grp)
    parts = []
    for stages in plan:
        acc = rest.pop(0)
        recvs = [rest.pop(0) for _ in stages]
        parts.append(Halving(stages, acc, recvs, rest.pop(0), rest.pop(0)))
    grams = []
    for stages, full in zip(gplan, (full_a, full_b)):
        acc = rest.pop(0)
        recvs = [rest.pop(0) for _ in stages]
        grams.append(Halving(stages, acc, recvs, *[rest.pop(0) for _ in range(2)], full,
                             *[rest.pop(0) for _ in range(2)]))
    barrier_all(gplan[0])
    masked, chosen = load_columns(idx_ref, cnt_ref, prior_ref, block_ref)
    rh, rl = split(jnp.concatenate([masked, chosen], axis=1))
    sk, width = sketch_ref.shape[0], rh.shape[1]
    per = sk // n
    step = 512
    flat = [[g[0] for g in stages] for stages in plan]
    for lane in range(0, width, 2 * T):
        wide = min(2 * T, width - lane)
        for r in range(0, sk, step):
            if lane == 0:
                h, l = split(sketch_ref[r:r + step, :])
                high[r:r + step, :] = h
                low[r:r + step, :] = l
            pair = (high[r:r + step, :], low[r:r + step, :])
            prod = dot3(pair, (rh[:, lane:lane + wide], rl[:, lane:lane + wide]))
            for j in range(wide // T):
                q = lane // T + j
                spots = block_at(flat[q], flat[0], n)
                for blk in range(r // per, (r + step) // per):
                    s = spots[blk] * per
                    parts[q].acc[s:s + per, :] = prod[blk * per - r:(blk + 1) * per - r, j * T:(j + 1) * T]
        for j in range(wide // T):
            parts[lane // T + j].start(0)
    for i in range(len(plan[0])):
        for part in parts:
            part.finish(i)
            if i + 1 < len(plan[0]):
                part.start(i + 1)
    mine = jnp.concatenate([part.acc[rows_at(part.off, per)] for part in parts], axis=1)
    t = 0
    for i in range(width // T):
        strip = dot(mine[:, i * T:(i + 1) * T], mine[:, :(i + 1) * T], 0, 0)
        for j in range(i + 1):
            q, s = t // 8, (t % 8) * T
            grams[q].acc[s:s + T, :] = strip[:, j * T:(j + 1) * T]
            t += 1
        if t >= 8 and t - i - 1 < 8 and grows == 8 * T:
            grams[0].start(0)
    for q in range(2):
        used = min(8, t - q * 8) * T
        if used < grows:
            grams[q].acc[used:grows, :] = jnp.zeros((grows - used, T), F32)
        if q or grows > 8 * T:
            grams[q].start(0)
    k = len(gplan[0])
    for i in range(k):
        for g in grams:
            g.finish(i)
            if i + 1 < k:
                g.start(i + 1)
            else:
                at = rows_at(g.off, g.size)
                g.full[at] = g.acc[at]
                g.gstart(k - 1)
    for i in range(k - 1, -1, -1):
        for g in grams:
            g.gfinish()
            if i:
                g.gstart(i - 1)


def sweep4(tiles, p, inverse):
    v, o = p // 8, p % 8
    lane = lax.broadcasted_iota(jnp.int32, (8, T), 1)
    sub = lax.broadcasted_iota(jnp.int32, (8, T), 0)
    r = [jnp.broadcast_to(tiles[v][o + i:o + i + 1, :], (8, T)) for i in range(4)]

    def at(i, j):
        return jnp.broadcast_to(r[i][:, p + j:p + j + 1], (8, T))

    a, b, e, f = at(0, 0), at(0, 1), at(0, 2), at(0, 3)
    c, g, h = at(1, 1), at(1, 2), at(1, 3)
    x, y, z = at(2, 2), at(2, 3), at(3, 3)
    ra = 1.0 / (a * c - b * b)
    k00, k01 = (c * e - b * g) * ra, (c * f - b * h) * ra
    k10, k11 = (a * g - b * e) * ra, (a * h - b * f) * ra
    s00 = x - (e * k00 + g * k10)
    s01 = y - (e * k01 + g * k11)
    s11 = z - (f * k01 + h * k11)
    rs = 1.0 / (s00 * s11 - s01 * s01)
    inside = (lane >= p) & (lane < p + 4)
    if inverse:
        r = [jnp.where(inside, jnp.where(lane == p + i, 1.0, 0.0), r[i]) for i in range(4)]
    g0, g1 = (c * r[0] - b * r[1]) * ra, (a * r[1] - b * r[0]) * ra
    q2 = r[2] - (k00 * r[0] + k10 * r[1])
    q3 = r[3] - (k01 * r[0] + k11 * r[1])
    n2, n3 = (s11 * q2 - s01 * q3) * rs, (s00 * q3 - s01 * q2) * rs
    n0, n1 = g0 - (k00 * n2 + k01 * n3), g1 - (k10 * n2 + k11 * n3)
    new = []
    for u, tile in enumerate(tiles):
        w = jnp.where(inside, 0.0, tile) if inverse else tile
        for j, row in enumerate((n0, n1, n2, n3)):
            w = w - tile[:, p + j:p + j + 1] * row
        if u == v:
            for j, row in enumerate((n0, n1, n2, n3)):
                w = jnp.where(sub == o + j, row, w)
        new.append(w)
    return new


def solve_kernel(idx_ref, cnt_ref, prior_ref, block_ref, ta_ref, tb_ref,
                 coef_ref, x_ref, resid_ref, gram_ref, a_ref, inv_ref):
    width = prior_ref.shape[1]
    blocks = width // T + 1
    t = 0
    for i in range(blocks):
        for j in range(i + 1):
            src, s = (ta_ref, t * T) if t < 8 else (tb_ref, (t - 8) * T)
            tile = src[s:s + T, :]
            if i == j and i < blocks - 1:
                row = lax.broadcasted_iota(jnp.int32, (T, T), 0)
                col = lax.broadcasted_iota(jnp.int32, (T, T), 1)
                tile = tile + jnp.where((row == col) & (row + i * T >= cnt_ref[0]), 1.0, 0.0)
            a_ref[i * T:(i + 1) * T, j * T:(j + 1) * T] = tile
            if i != j:
                a_ref[j * T:(j + 1) * T, i * T:(i + 1) * T] = tile.T
            t += 1

    def body(k, _):
        at = pl.ds(pl.multiple_of(k * T, T), T)
        d = a_ref[at, at]
        tiles = [d[8 * v:8 * v + 8, :] for v in range(T // 8)]
        for p in range(0, T, 4):
            tiles = sweep4(tiles, p, True)
        inv_ref[...] = jnp.concatenate(tiles, axis=0)
        for kk in range(blocks - 1):
            @pl.when(k == kk)
            def _():
                own, rest = slice(kk * T, (kk + 1) * T), slice((kk + 1) * T, blocks * T)
                rowk = dot(inv_ref[...], a_ref[own, rest])
                if kk:
                    top = slice(0, kk * T)
                    a_ref[top, rest] = a_ref[top, rest] - dot(a_ref[top, own], rowk)
                a_ref[rest, rest] = a_ref[rest, rest] - dot(a_ref[rest, own], rowk)
                a_ref[own, rest] = rowk
        return 0

    lax.fori_loop(0, blocks - 1, body, 0)
    coef = a_ref[0:width, width:width + T]
    coef_ref[...] = coef
    e = a_ref[width:width + P_SIZE, width:width + T]
    tiles = [e[8 * v:8 * v + 8, :] for v in range(P_SIZE // 8)]
    for p in range(0, P_SIZE, 4):
        tiles = sweep4(tiles, p, False)
    x = jnp.concatenate(tiles, axis=0)[:, P_SIZE:]
    x_ref[...] = x
    masked, chosen = load_columns(idx_ref, cnt_ref, prior_ref, block_ref)
    resid = chosen - dot(masked, coef)
    one = resid[:, :P_SIZE]
    two = resid[:, P_SIZE:] - dot(one, x)
    resid_ref[...] = jnp.concatenate([one, two], axis=1)
    gram_ref[...] = jnp.concatenate([dot(one, one, 0, 0), dot(two, two, 0, 0)], axis=1)


def sum_kernel(rows, grp, gram_ref, out_ref, half, *rest):
    stages = gram_plan(rows, grp)[0]
    core, wide = stages[0], stages[1:]
    slots, holds = rest[:len(wide)], rest[len(wide):2 * len(wide)]
    send_sem, recv_sem = rest[2 * len(wide):]
    barrier_all(stages)
    size = gram_ref.shape[0] // 2
    mine = rows_at(spot_in(core) * size, size)
    c = remote(gram_ref.at[rows_at(spot_in(core, 1) * size, size)], half, send_sem.at[0, 0],
               recv_sem.at[0, 0], core, 1)
    c.start()
    c.wait()
    total = gram_ref[mine, :] + half[...]
    for i, group in enumerate(wide):
        src = holds[i]
        src[...] = total
        here = spot_in(group)
        pend = []
        for m in range(1, 1 << len(group)):
            c = remote(src, slots[i].at[here], send_sem.at[i + 1, m - 1], recv_sem.at[i + 1, m - 1], group, m)
            c.start()
            pend.append(c)
        slots[i][here] = total
        for c in pend:
            c.wait()
        total = slots[i][0]
        for m in range(1, 1 << len(group)):
            total = total + slots[i][m]
    out_ref[mine, :] = total
    k = len(stages)
    c = remote(out_ref.at[mine], out_ref.at[mine], send_sem.at[k, 0], recv_sem.at[k, 0], core, 1)
    c.start()
    c.wait()


def finish_kernel(scale, gram_ref, resid_ref, x_ref, coef_ref, basis_ref, factors_ref):
    gram = gram_ref[...]
    eye = (lax.broadcasted_iota(jnp.int32, (P_SIZE, P_SIZE), 0)
           == lax.broadcasted_iota(jnp.int32, (P_SIZE, P_SIZE), 1)).astype(F32)
    sub = lax.broadcasted_iota(jnp.int32, (8, T), 0)
    mats = []
    for h in range(2):
        m = jnp.concatenate([gram[:, h * P_SIZE:(h + 1) * P_SIZE], eye], axis=1)
        mats.append([m[8 * v:8 * v + 8, :] for v in range(P_SIZE // 8)])
    for p in range(P_SIZE):
        v, o = p // 8, p % 8
        for h in range(2):
            tiles = mats[h]
            row = tiles[v][o:o + 1, :]
            d = row[:, p:p + 1]
            y = lax.rsqrt(d)
            y = y * (1.5 - 0.5 * d * y * y)
            row = row * y
            new = list(tiles)
            for u in range(v, P_SIZE // 8):
                w = tiles[u] - (tiles[u][:, p:p + 1] * y) * row
                if u == v:
                    w = jnp.where(sub == o, row, jnp.where(sub > o, w, tiles[u]))
                new[u] = w
            mats[h] = new
    full = [jnp.concatenate(m, axis=0) for m in mats]
    row = lax.broadcasted_iota(jnp.int32, (P_SIZE, P_SIZE), 0)
    col = lax.broadcasted_iota(jnp.int32, (P_SIZE, P_SIZE), 1)
    upper = [jnp.where(row <= col, f[:, :P_SIZE], 0.0) for f in full]
    lowinv = [f[:, P_SIZE:] for f in full]
    basis_ref[...] = jnp.concatenate(
        [dot(resid_ref[:, h * P_SIZE:(h + 1) * P_SIZE], lowinv[h], 1, 1) for h in range(2)], axis=1
    ) * scale
    width = coef_ref.shape[0]
    factors_ref[0:width, :] = coef_ref[...]
    inner = dot(upper[0], x_ref[...])
    factors_ref[width:width + P_SIZE, :] = jnp.concatenate([upper[0], inner], axis=1)
    factors_ref[width + P_SIZE:, :] = jnp.concatenate([jnp.zeros_like(eye), upper[1]], axis=1)


def shards(rows, grp, sketch, prior, block, idx, cnt):
    n = rows * grp
    sk, local = sketch.shape
    width = prior.shape[1]
    vm = pl.BlockSpec(memory_space=pltpu.VMEM)
    sm = pl.BlockSpec(memory_space=pltpu.SMEM)
    grows = n * max(8, 8 * T // n)
    scratch = [pltpu.VMEM((sk, local), jnp.bfloat16)] * 2
    for stages in sketch_plan(rows, grp):
        scratch += [pltpu.VMEM((sk, T), F32)] + recv_shapes(stages, sk, T) + [sem_shape(stages)] * 2
    for stages in gram_plan(rows, grp):
        scratch += [pltpu.VMEM((grows, T), F32)] + recv_shapes(stages, grows, T) + [sem_shape(stages)] * 4
    tiles = pl.pallas_call(
        functools.partial(gram_kernel, rows, grp, grows),
        out_shape=[jax.ShapeDtypeStruct((grows, T), F32)] * 2,
        in_specs=[sm, sm, vm, vm, vm],
        out_specs=[vm, vm],
        scratch_shapes=scratch,
        compiler_params=pltpu.CompilerParams(
            collective_id=0, has_side_effects=True, vmem_limit_bytes=VMEM_LIMIT
        ),
    )(idx, cnt, sketch, prior, block)
    coef, x, resid, gram = pl.pallas_call(
        solve_kernel,
        out_shape=[
            jax.ShapeDtypeStruct((width, T), F32),
            jax.ShapeDtypeStruct((P_SIZE, P_SIZE), F32),
            jax.ShapeDtypeStruct((local, T), F32),
            jax.ShapeDtypeStruct((P_SIZE, T), F32),
        ],
        in_specs=[sm, sm, vm, vm, vm, vm],
        out_specs=[vm] * 4,
        scratch_shapes=[pltpu.VMEM((width + T, width + T), F32), pltpu.VMEM((T, T), F32)],
        compiler_params=pltpu.CompilerParams(vmem_limit_bytes=VMEM_LIMIT),
    )(idx, cnt, prior, block, *tiles)
    scale = float(local * n) ** 0.5
    stages = gram_plan(rows, grp)[0]
    half = P_SIZE // 2
    most = max((1 << len(g)) - 1 for g in stages)
    gram = pl.pallas_call(
        functools.partial(sum_kernel, rows, grp),
        out_shape=jax.ShapeDtypeStruct((P_SIZE, T), F32),
        in_specs=[vm],
        out_specs=vm,
        scratch_shapes=[pltpu.VMEM((half, T), F32)]
        + [pltpu.VMEM((1 << len(g), half, T), F32) for g in stages[1:]]
        + [pltpu.VMEM((half, T), F32) for g in stages[1:]]
        + [pltpu.SemaphoreType.DMA((len(stages) + 1, most))] * 2,
        compiler_params=pltpu.CompilerParams(collective_id=1, has_side_effects=True),
    )(gram)
    return tuple(pl.pallas_call(
        functools.partial(finish_kernel, scale),
        out_shape=[
            jax.ShapeDtypeStruct((local, T), F32),
            jax.ShapeDtypeStruct((width + T, T), F32),
        ],
        in_specs=[vm] * 4,
        out_specs=[vm] * 2,
        compiler_params=pltpu.CompilerParams(vmem_limit_bytes=VMEM_LIMIT),
    )(gram, resid, x, coef))


def solution(mesh):
    rows, grp = mesh.shape["rows"], mesh.shape["grp"]
    placed = (
        P(None, ("rows", "grp")),
        P(("rows", "grp"), None),
        P(("rows", "grp"), None),
        P(),
        P(),
    )
    return jax.shard_map(
        functools.partial(shards, rows, grp),
        mesh=mesh,
        in_specs=placed,
        out_specs=(P(("rows", "grp"), None), P()),
        check_vma=False,
    )
```

```python
import functools

import jax
import jax.numpy as jnp
from jax import lax
from jax.experimental import pallas as pl
from jax.experimental.pallas import tpu as pltpu
from jax.sharding import PartitionSpec as P

P_SIZE = 64
T = 128
HIGHEST = lax.Precision.HIGHEST
F32 = jnp.float32
VMEM_LIMIT = 60 * 1024 * 1024


def dot(a, b, ca=1, cb=0):
    return lax.dot_general(
        a, b, (((ca,), (cb,)), ((), ())), precision=HIGHEST, preferred_element_type=F32
    )


def split(x):
    hi = x.astype(jnp.bfloat16)
    return hi, (x - hi.astype(F32)).astype(jnp.bfloat16)


def dot3(a, b):
    ah, al = a
    bh, bl = b
    out = jnp.dot(ah, bl, preferred_element_type=F32)
    out = out + jnp.dot(al, bh, preferred_element_type=F32)
    return out + jnp.dot(ah, bh, preferred_element_type=F32)


def bits_of(size):
    out, b = [], 1
    while b < size:
        out.append(b)
        b *= 2
    return out


def axes_of(rows, grp):
    core = [("grp", b) for b in bits_of(grp)[:1]]
    y = [("grp", b) for b in bits_of(grp)[1:]]
    x = [("rows", b) for b in bits_of(rows)[:1]]
    z = [("rows", b) for b in bits_of(rows)[1:]]
    return core, y, x, z


def my_bit(axis, b):
    return (lax.axis_index(axis) // b) % 2


def peer(group, pattern):
    out = {}
    for i, (axis, b) in enumerate(group):
        if (pattern >> (len(group) - 1 - i)) & 1:
            here = out.get(axis, lax.axis_index(axis))
            out[axis] = here + b * (1 - 2 * my_bit(axis, b))
    return out


def spot_in(group, pattern=0):
    k, at = len(group), 0
    for i, (axis, b) in enumerate(group):
        flip, bit = (pattern >> (k - 1 - i)) & 1, my_bit(axis, b)
        at = at + (1 - bit if flip else bit) * (1 << (k - 1 - i))
    return at


def barrier_all(groups):
    sem = pltpu.get_barrier_semaphore()
    count = 0
    for group in groups:
        for pattern in range(1, 1 << len(group)):
            pl.semaphore_signal(
                sem, inc=1, device_id=peer(group, pattern), device_id_type=pl.DeviceIdType.MESH
            )
            count += 1
    pl.semaphore_wait(sem, count)


def remote(src, dst, send, recv, group, pattern):
    return pltpu.make_async_remote_copy(
        src_ref=src, dst_ref=dst, send_sem=send, recv_sem=recv,
        device_id=peer(group, pattern), device_id_type=pl.DeviceIdType.MESH,
    )


def rows_at(start, size):
    return pl.ds(pl.multiple_of(start, 8), size)


class Halving:
    def __init__(self, stages, acc, recvs, sends, arrives, full=None, gsends=None, garrives=None):
        self.stages, self.acc, self.recvs, self.full = stages, acc, recvs, full
        self.sems, self.gsems = (sends, arrives), (gsends, garrives)
        self.off, self.size, self.pend = 0, acc.shape[0], []

    def start(self, i):
        group = self.stages[i]
        sub = self.size >> len(group)
        self.pend = []
        for m in range(1, 1 << len(group)):
            src = self.acc.at[rows_at(self.off + spot_in(group, m) * sub, sub)]
            c = remote(src, self.recvs[i].at[m - 1], self.sems[0].at[i, m - 1],
                       self.sems[1].at[i, m - 1], group, m)
            c.start()
            self.pend.append(c)
        self.off = self.off + spot_in(group) * sub
        self.size = sub

    def finish(self, i):
        for c in self.pend:
            c.wait()
        at = rows_at(self.off, self.size)
        total = self.acc[at]
        for m in range(len(self.pend)):
            total = total + self.recvs[i][m]
        self.acc[at] = total

    def gstart(self, i):
        group = self.stages[i]
        self.pend = []
        at = self.full.at[rows_at(self.off, self.size)]
        for m in range(1, 1 << len(group)):
            c = remote(at, at, self.gsems[0].at[i, m - 1], self.gsems[1].at[i, m - 1], group, m)
            c.start()
            self.pend.append(c)
        self.off = self.off - spot_in(group) * self.size
        self.size = self.size << len(group)

    def gfinish(self):
        for c in self.pend:
            c.wait()


def recv_shapes(stages, rows, lanes):
    out = []
    for group in stages:
        rows = rows >> len(group)
        out.append(pltpu.VMEM(((1 << len(group)) - 1, rows, lanes), F32))
    return out


def sem_shape(stages):
    return pltpu.SemaphoreType.DMA((len(stages), max((1 << len(g)) - 1 for g in stages)))


def sketch_plan(rows, grp):
    core, y, x, z = axes_of(rows, grp)
    one = lambda bits: [[b] for b in bits]
    first, second, third = one(core + x + y + z), one(core + y + x + z), one(core + z + x + y)
    return [first, second, third, first, second]


def gram_plan(rows, grp):
    core, y, x, z = axes_of(rows, grp)
    return [[g for g in (core, x + y, z) if g], [g for g in (core, z, x + y) if g]]


def block_at(order, target, n):
    k = len(order)
    spots = []
    for blk in range(n):
        value = {target[i]: (blk >> (k - 1 - i)) & 1 for i in range(k)}
        spots.append(sum(value[order[i]] << (k - 1 - i) for i in range(k)))
    return spots


def load_columns(idx_ref, cnt_ref, prior_ref, block_ref):
    width = prior_ref.shape[1]
    lane = lax.broadcasted_iota(jnp.int32, prior_ref.shape, 1)
    masked = jnp.where(lane < cnt_ref[0], prior_ref[...], 0.0)
    start = idx_ref[0]
    chosen = block_ref[:, 0:2 * P_SIZE]
    for s in range(1, block_ref.shape[1] // P_SIZE - 1):
        chosen = jnp.where(start == s, block_ref[:, s * P_SIZE:(s + 2) * P_SIZE], chosen)
    return masked, chosen


def gram_kernel(rows, grp, grows, idx_ref, cnt_ref, sketch_ref, prior_ref, block_ref,
                full_a, full_b, *rest):
    rest = list(rest)
    n = rows * grp
    high, low = rest.pop(0), rest.pop(0)
    plan, gplan = sketch_plan(rows, grp), gram_plan(rows, grp)
    parts = []
    for stages in plan:
        acc = rest.pop(0)
        recvs = [rest.pop(0) for _ in stages]
        parts.append(Halving(stages, acc, recvs, rest.pop(0), rest.pop(0)))
    grams = []
    for stages, full in zip(gplan, (full_a, full_b)):
        acc = rest.pop(0)
        recvs = [rest.pop(0) for _ in stages]
        grams.append(Halving(stages, acc, recvs, *[rest.pop(0) for _ in range(2)], full,
                             *[rest.pop(0) for _ in range(2)]))
    barrier_all(gplan[0])
    masked, chosen = load_columns(idx_ref, cnt_ref, prior_ref, block_ref)
    rh, rl = split(jnp.concatenate([masked, chosen], axis=1))
    sk, width = sketch_ref.shape[0], rh.shape[1]
    per = sk // n
    step = 512
    flat = [[g[0] for g in stages] for stages in plan]
    for lane in range(0, width, 2 * T):
        wide = min(2 * T, width - lane)
        for r in range(0, sk, step):
            if lane == 0:
                h, l = split(sketch_ref[r:r + step, :])
                high[r:r + step, :] = h
                low[r:r + step, :] = l
            pair = (high[r:r + step, :], low[r:r + step, :])
            prod = dot3(pair, (rh[:, lane:lane + wide], rl[:, lane:lane + wide]))
            for j in range(wide // T):
                q = lane // T + j
                spots = block_at(flat[q], flat[0], n)
                for blk in range(r // per, (r + step) // per):
                    s = spots[blk] * per
                    parts[q].acc[s:s + per, :] = prod[blk * per - r:(blk + 1) * per - r, j * T:(j + 1) * T]
        for j in range(wide // T):
            parts[lane // T + j].start(0)
    for i in range(len(plan[0])):
        for part in parts:
            part.finish(i)
            if i + 1 < len(plan[0]):
                part.start(i + 1)
    mine = jnp.concatenate([part.acc[rows_at(part.off, per)] for part in parts], axis=1)
    t = 0
    for i in range(width // T):
        strip = dot(mine[:, i * T:(i + 1) * T], mine[:, :(i + 1) * T], 0, 0)
        for j in range(i + 1):
            q, s = t // 8, (t % 8) * T
            grams[q].acc[s:s + T, :] = strip[:, j * T:(j + 1) * T]
            t += 1
        if t >= 8 and t - i - 1 < 8 and grows == 8 * T:
            grams[0].start(0)
    for q in range(2):
        used = min(8, t - q * 8) * T
        if used < grows:
            grams[q].acc[used:grows, :] = jnp.zeros((grows - used, T), F32)
        if q or grows > 8 * T:
            grams[q].start(0)
    k = len(gplan[0])
    for i in range(k):
        for g in grams:
            g.finish(i)
            if i + 1 < k:
                g.start(i + 1)
            else:
                at = rows_at(g.off, g.size)
                g.full[at] = g.acc[at]
                g.gstart(k - 1)
    for i in range(k - 1, -1, -1):
        for g in grams:
            g.gfinish()
            if i:
                g.gstart(i - 1)


def solve4(tile, p, sides):
    o = p % 8

    def spread(t):
        return [jnp.broadcast_to(t[o + i:o + i + 1, :], (8, T)) for i in range(4)]

    own = spread(tile)

    def at(i, j):
        return jnp.broadcast_to(own[i][:, p + j:p + j + 1], (8, T))

    a, b, e, f = at(0, 0), at(0, 1), at(0, 2), at(0, 3)
    c, g, h = at(1, 1), at(1, 2), at(1, 3)
    x, y, z = at(2, 2), at(2, 3), at(3, 3)
    ra = 1.0 / (a * c - b * b)
    k00, k01 = (c * e - b * g) * ra, (c * f - b * h) * ra
    k10, k11 = (a * g - b * e) * ra, (a * h - b * f) * ra
    s00 = x - (e * k00 + g * k10)
    s01 = y - (e * k01 + g * k11)
    s11 = z - (f * k01 + h * k11)
    rs = 1.0 / (s00 * s11 - s01 * s01)
    out = []
    for side in sides:
        r = spread(side)
        g0, g1 = (c * r[0] - b * r[1]) * ra, (a * r[1] - b * r[0]) * ra
        q2 = r[2] - (k00 * r[0] + k10 * r[1])
        q3 = r[3] - (k01 * r[0] + k11 * r[1])
        n2, n3 = (s11 * q2 - s01 * q3) * rs, (s00 * q3 - s01 * q2) * rs
        out.append([g0 - (k00 * n2 + k01 * n3), g1 - (k10 * n2 + k11 * n3), n2, n3])
    return out


def put4(tile, p, rows):
    sub = lax.broadcasted_iota(jnp.int32, (8, T), 0)
    for j, row in enumerate(rows):
        tile = jnp.where(sub == p % 8 + j, row, tile)
    return tile


def eliminate4(tiles, p):
    v = p // 8
    rows, = solve4(tiles[v], p, [tiles[v]])
    new = []
    for u, w in enumerate(tiles):
        tile = w
        for j in range(4):
            w = w - tile[:, p + j:p + j + 1] * rows[j]
        new.append(put4(w, p, rows) if u == v else w)
    return new


def factor4(mat, low, norm, p):
    v, o = p // 8, p % 8
    sub = lax.broadcasted_iota(jnp.int32, (8, T), 0)
    rows, lows = solve4(mat[v], p, [mat[v], low[v]])
    norm[v] = put4(norm[v], p, lows)
    for u in range(v if o == 0 else v + 1, len(mat)):
        w, l = mat[u], low[u]
        for j in range(4):
            col = jnp.broadcast_to(mat[u][:, p + j:p + j + 1], (8, T))
            w = w - col * rows[j]
            l = l - col * lows[j]
        if u == v:
            w, l = jnp.where(sub >= 4, w, mat[u]), jnp.where(sub >= 4, l, low[u])
        mat[u], low[u] = w, l


def solve_kernel(idx_ref, cnt_ref, prior_ref, block_ref, ta_ref, tb_ref,
                 coef_ref, x_ref, resid_ref, gram_ref, a_ref, inv_ref):
    width = prior_ref.shape[1]
    blocks = width // T + 1
    t = 0
    for i in range(blocks):
        for j in range(i + 1):
            src, s = (ta_ref, t * T) if t < 8 else (tb_ref, (t - 8) * T)
            tile = src[s:s + T, :]
            if i == j and i < blocks - 1:
                row = lax.broadcasted_iota(jnp.int32, (T, T), 0)
                col = lax.broadcasted_iota(jnp.int32, (T, T), 1)
                tile = tile + jnp.where((row == col) & (row + i * T >= cnt_ref[0]), 1.0, 0.0)
            a_ref[i * T:(i + 1) * T, j * T:(j + 1) * T] = tile
            if i != j:
                a_ref[j * T:(j + 1) * T, i * T:(i + 1) * T] = tile.T
            t += 1

    def body(k, _):
        at = pl.ds(pl.multiple_of(k * T, T), T)
        d = a_ref[at, at]
        mat = [d[8 * v:8 * v + 8, :] for v in range(T // 8)]
        lane = lax.broadcasted_iota(jnp.int32, (8, T), 1)
        sub = lax.broadcasted_iota(jnp.int32, (8, T), 0)
        low = [jnp.where(lane == sub + 8 * v, 1.0, 0.0) for v in range(T // 8)]
        norm = [jnp.zeros((8, T), F32) for v in range(T // 8)]
        for p in range(0, T, 4):
            factor4(mat, low, norm, p)
        inv_ref[...] = dot(jnp.concatenate(low, axis=0), jnp.concatenate(norm, axis=0), 0, 0)
        for kk in range(blocks - 1):
            @pl.when(k == kk)
            def _():
                own, rest = slice(kk * T, (kk + 1) * T), slice((kk + 1) * T, blocks * T)
                rowk = dot(inv_ref[...], a_ref[own, rest])
                if kk:
                    top = slice(0, kk * T)
                    a_ref[top, rest] = a_ref[top, rest] - dot(a_ref[top, own], rowk)
                a_ref[rest, rest] = a_ref[rest, rest] - dot(a_ref[rest, own], rowk)
                a_ref[own, rest] = rowk
        return 0

    lax.fori_loop(0, blocks - 1, body, 0)
    coef = a_ref[0:width, width:width + T]
    coef_ref[...] = coef
    e = a_ref[width:width + P_SIZE, width:width + T]
    tiles = [e[8 * v:8 * v + 8, :] for v in range(P_SIZE // 8)]
    for p in range(0, P_SIZE, 4):
        tiles = eliminate4(tiles, p)
    x = jnp.concatenate(tiles, axis=0)[:, P_SIZE:]
    x_ref[...] = x
    masked, chosen = load_columns(idx_ref, cnt_ref, prior_ref, block_ref)
    resid = chosen - dot(masked, coef)
    one = resid[:, :P_SIZE]
    two = resid[:, P_SIZE:] - dot(one, x)
    resid_ref[...] = jnp.concatenate([one, two], axis=1)
    gram_ref[...] = jnp.concatenate([dot(one, one, 0, 0), dot(two, two, 0, 0)], axis=1)


def sum_kernel(rows, grp, gram_ref, out_ref, half, *rest):
    stages = gram_plan(rows, grp)[0]
    core, wide = stages[0], stages[1:]
    slots, holds = rest[:len(wide)], rest[len(wide):2 * len(wide)]
    send_sem, recv_sem = rest[2 * len(wide):]
    barrier_all(stages)
    size = gram_ref.shape[0] // 2
    mine = rows_at(spot_in(core) * size, size)
    c = remote(gram_ref.at[rows_at(spot_in(core, 1) * size, size)], half, send_sem.at[0, 0],
               recv_sem.at[0, 0], core, 1)
    c.start()
    c.wait()
    total = gram_ref[mine, :] + half[...]
    for i, group in enumerate(wide):
        src = holds[i]
        src[...] = total
        here = spot_in(group)
        pend = []
        for m in range(1, 1 << len(group)):
            c = remote(src, slots[i].at[here], send_sem.at[i + 1, m - 1], recv_sem.at[i + 1, m - 1], group, m)
            c.start()
            pend.append(c)
        slots[i][here] = total
        for c in pend:
            c.wait()
        total = slots[i][0]
        for m in range(1, 1 << len(group)):
            total = total + slots[i][m]
    out_ref[mine, :] = total
    k = len(stages)
    c = remote(out_ref.at[mine], out_ref.at[mine], send_sem.at[k, 0], recv_sem.at[k, 0], core, 1)
    c.start()
    c.wait()


def finish_kernel(scale, gram_ref, resid_ref, x_ref, coef_ref, basis_ref, factors_ref):
    gram = gram_ref[...]
    eye = (lax.broadcasted_iota(jnp.int32, (P_SIZE, P_SIZE), 0)
           == lax.broadcasted_iota(jnp.int32, (P_SIZE, P_SIZE), 1)).astype(F32)
    sub = lax.broadcasted_iota(jnp.int32, (8, T), 0)
    mats = []
    for h in range(2):
        m = jnp.concatenate([gram[:, h * P_SIZE:(h + 1) * P_SIZE], eye], axis=1)
        mats.append([m[8 * v:8 * v + 8, :] for v in range(P_SIZE // 8)])
    for p in range(P_SIZE):
        v, o = p // 8, p % 8
        for h in range(2):
            tiles = mats[h]
            row = tiles[v][o:o + 1, :]
            d = row[:, p:p + 1]
            y = lax.rsqrt(d)
            y = y * (1.5 - 0.5 * d * y * y)
            row = row * y
            new = list(tiles)
            for u in range(v, P_SIZE // 8):
                w = tiles[u] - (tiles[u][:, p:p + 1] * y) * row
                if u == v:
                    w = jnp.where(sub == o, row, jnp.where(sub > o, w, tiles[u]))
                new[u] = w
            mats[h] = new
    full = [jnp.concatenate(m, axis=0) for m in mats]
    row = lax.broadcasted_iota(jnp.int32, (P_SIZE, P_SIZE), 0)
    col = lax.broadcasted_iota(jnp.int32, (P_SIZE, P_SIZE), 1)
    upper = [jnp.where(row <= col, f[:, :P_SIZE], 0.0) for f in full]
    lowinv = [f[:, P_SIZE:] for f in full]
    basis_ref[...] = jnp.concatenate(
        [dot(resid_ref[:, h * P_SIZE:(h + 1) * P_SIZE], lowinv[h], 1, 1) for h in range(2)], axis=1
    ) * scale
    width = coef_ref.shape[0]
    factors_ref[0:width, :] = coef_ref[...]
    inner = dot(upper[0], x_ref[...])
    factors_ref[width:width + P_SIZE, :] = jnp.concatenate([upper[0], inner], axis=1)
    factors_ref[width + P_SIZE:, :] = jnp.concatenate([jnp.zeros_like(eye), upper[1]], axis=1)


def shards(rows, grp, sketch, prior, block, idx, cnt):
    n = rows * grp
    sk, local = sketch.shape
    width = prior.shape[1]
    vm = pl.BlockSpec(memory_space=pltpu.VMEM)
    sm = pl.BlockSpec(memory_space=pltpu.SMEM)
    grows = n * max(8, 8 * T // n)
    scratch = [pltpu.VMEM((sk, local), jnp.bfloat16)] * 2
    for stages in sketch_plan(rows, grp):
        scratch += [pltpu.VMEM((sk, T), F32)] + recv_shapes(stages, sk, T) + [sem_shape(stages)] * 2
    for stages in gram_plan(rows, grp):
        scratch += [pltpu.VMEM((grows, T), F32)] + recv_shapes(stages, grows, T) + [sem_shape(stages)] * 4
    tiles = pl.pallas_call(
        functools.partial(gram_kernel, rows, grp, grows),
        out_shape=[jax.ShapeDtypeStruct((grows, T), F32)] * 2,
        in_specs=[sm, sm, vm, vm, vm],
        out_specs=[vm, vm],
        scratch_shapes=scratch,
        compiler_params=pltpu.CompilerParams(
            collective_id=0, has_side_effects=True, vmem_limit_bytes=VMEM_LIMIT
        ),
    )(idx, cnt, sketch, prior, block)
    coef, x, resid, gram = pl.pallas_call(
        solve_kernel,
        out_shape=[
            jax.ShapeDtypeStruct((width, T), F32),
            jax.ShapeDtypeStruct((P_SIZE, P_SIZE), F32),
            jax.ShapeDtypeStruct((local, T), F32),
            jax.ShapeDtypeStruct((P_SIZE, T), F32),
        ],
        in_specs=[sm, sm, vm, vm, vm, vm],
        out_specs=[vm] * 4,
        scratch_shapes=[pltpu.VMEM((width + T, width + T), F32), pltpu.VMEM((T, T), F32)],
        compiler_params=pltpu.CompilerParams(vmem_limit_bytes=VMEM_LIMIT),
    )(idx, cnt, prior, block, *tiles)
    scale = float(local * n) ** 0.5
    stages = gram_plan(rows, grp)[0]
    half = P_SIZE // 2
    most = max((1 << len(g)) - 1 for g in stages)
    gram = pl.pallas_call(
        functools.partial(sum_kernel, rows, grp),
        out_shape=jax.ShapeDtypeStruct((P_SIZE, T), F32),
        in_specs=[vm],
        out_specs=vm,
        scratch_shapes=[pltpu.VMEM((half, T), F32)]
        + [pltpu.VMEM((1 << len(g), half, T), F32) for g in stages[1:]]
        + [pltpu.VMEM((half, T), F32) for g in stages[1:]]
        + [pltpu.SemaphoreType.DMA((len(stages) + 1, most))] * 2,
        compiler_params=pltpu.CompilerParams(collective_id=1, has_side_effects=True),
    )(gram)
    return tuple(pl.pallas_call(
        functools.partial(finish_kernel, scale),
        out_shape=[
            jax.ShapeDtypeStruct((local, T), F32),
            jax.ShapeDtypeStruct((width + T, T), F32),
        ],
        in_specs=[vm] * 4,
        out_specs=[vm] * 2,
        compiler_params=pltpu.CompilerParams(vmem_limit_bytes=VMEM_LIMIT),
    )(gram, resid, x, coef))


def solution(mesh):
    rows, grp = mesh.shape["rows"], mesh.shape["grp"]
    placed = (
        P(None, ("rows", "grp")),
        P(("rows", "grp"), None),
        P(("rows", "grp"), None),
        P(),
        P(),
    )
    return jax.shard_map(
        functools.partial(shards, rows, grp),
        mesh=mesh,
        in_specs=placed,
        out_specs=(P(("rows", "grp"), None), P()),
        check_vma=False,
    )
```

```python
import functools

import jax
import jax.numpy as jnp
from jax import lax
from jax.experimental import pallas as pl
from jax.experimental.pallas import tpu as pltpu
from jax.sharding import PartitionSpec as P

P_SIZE = 64
T = 128
HIGHEST = lax.Precision.HIGHEST
F32 = jnp.float32
VMEM_LIMIT = 60 * 1024 * 1024


def dot(a, b, ca=1, cb=0):
    return lax.dot_general(
        a, b, (((ca,), (cb,)), ((), ())), precision=HIGHEST, preferred_element_type=F32
    )


def split(x):
    hi = x.astype(jnp.bfloat16)
    return hi, (x - hi.astype(F32)).astype(jnp.bfloat16)


def dot3(a, b):
    ah, al = a
    bh, bl = b
    out = jnp.dot(ah, bl, preferred_element_type=F32)
    out = out + jnp.dot(al, bh, preferred_element_type=F32)
    return out + jnp.dot(ah, bh, preferred_element_type=F32)


def bits_of(size):
    out, b = [], 1
    while b < size:
        out.append(b)
        b *= 2
    return out


def axes_of(rows, grp):
    core = [("grp", b) for b in bits_of(grp)[:1]]
    y = [("grp", b) for b in bits_of(grp)[1:]]
    x = [("rows", b) for b in bits_of(rows)[:1]]
    z = [("rows", b) for b in bits_of(rows)[1:]]
    return core, y, x, z


def my_bit(axis, b):
    return (lax.axis_index(axis) // b) % 2


def peer(group, pattern):
    out = {}
    for i, (axis, b) in enumerate(group):
        if (pattern >> (len(group) - 1 - i)) & 1:
            here = out.get(axis, lax.axis_index(axis))
            out[axis] = here + b * (1 - 2 * my_bit(axis, b))
    return out


def spot_in(group, pattern=0):
    k, at = len(group), 0
    for i, (axis, b) in enumerate(group):
        flip, bit = (pattern >> (k - 1 - i)) & 1, my_bit(axis, b)
        at = at + (1 - bit if flip else bit) * (1 << (k - 1 - i))
    return at


def barrier_all(groups):
    sem = pltpu.get_barrier_semaphore()
    count = 0
    for group in groups:
        for pattern in range(1, 1 << len(group)):
            pl.semaphore_signal(
                sem, inc=1, device_id=peer(group, pattern), device_id_type=pl.DeviceIdType.MESH
            )
            count += 1
    pl.semaphore_wait(sem, count)


def remote(src, dst, send, recv, group, pattern):
    return pltpu.make_async_remote_copy(
        src_ref=src, dst_ref=dst, send_sem=send, recv_sem=recv,
        device_id=peer(group, pattern), device_id_type=pl.DeviceIdType.MESH,
    )


def rows_at(start, size):
    return pl.ds(pl.multiple_of(start, 8), size)


class Halving:
    def __init__(self, stages, acc, recvs, sends, arrives, full=None, gsends=None, garrives=None):
        self.stages, self.acc, self.recvs, self.full = stages, acc, recvs, full
        self.sems, self.gsems = (sends, arrives), (gsends, garrives)
        self.off, self.size, self.pend = 0, acc.shape[0], []

    def start(self, i):
        group = self.stages[i]
        sub = self.size >> len(group)
        self.pend = []
        for m in range(1, 1 << len(group)):
            src = self.acc.at[rows_at(self.off + spot_in(group, m) * sub, sub)]
            c = remote(src, self.recvs[i].at[m - 1], self.sems[0].at[i, m - 1],
                       self.sems[1].at[i, m - 1], group, m)
            c.start()
            self.pend.append(c)
        self.off = self.off + spot_in(group) * sub
        self.size = sub

    def finish(self, i):
        for c in self.pend:
            c.wait()
        at = rows_at(self.off, self.size)
        total = self.acc[at]
        for m in range(len(self.pend)):
            total = total + self.recvs[i][m]
        self.acc[at] = total

    def gstart(self, i):
        group = self.stages[i]
        self.pend = []
        at = self.full.at[rows_at(self.off, self.size)]
        for m in range(1, 1 << len(group)):
            c = remote(at, at, self.gsems[0].at[i, m - 1], self.gsems[1].at[i, m - 1], group, m)
            c.start()
            self.pend.append(c)
        self.off = self.off - spot_in(group) * self.size
        self.size = self.size << len(group)

    def gfinish(self):
        for c in self.pend:
            c.wait()


def recv_shapes(stages, rows, lanes):
    out = []
    for group in stages:
        rows = rows >> len(group)
        out.append(pltpu.VMEM(((1 << len(group)) - 1, rows, lanes), F32))
    return out


def sem_shape(stages):
    return pltpu.SemaphoreType.DMA((len(stages), max((1 << len(g)) - 1 for g in stages)))


def sketch_plan(rows, grp):
    core, y, x, z = axes_of(rows, grp)
    one = lambda bits: [[b] for b in bits]
    first, second, third = one(core + x + y + z), one(core + y + x + z), one(core + z + x + y)
    return [first, second, third, first, second]


def gram_plan(rows, grp):
    core, y, x, z = axes_of(rows, grp)
    return [[g for g in (core, x + y, z) if g], [g for g in (core, x + y, z) if g]]


def block_at(order, target, n):
    k = len(order)
    spots = []
    for blk in range(n):
        value = {target[i]: (blk >> (k - 1 - i)) & 1 for i in range(k)}
        spots.append(sum(value[order[i]] << (k - 1 - i) for i in range(k)))
    return spots


def load_columns(idx_ref, cnt_ref, prior_ref, block_ref):
    width = prior_ref.shape[1]
    lane = lax.broadcasted_iota(jnp.int32, prior_ref.shape, 1)
    masked = jnp.where(lane < cnt_ref[0], prior_ref[...], 0.0)
    start = idx_ref[0]
    chosen = block_ref[:, 0:2 * P_SIZE]
    for s in range(1, block_ref.shape[1] // P_SIZE - 1):
        chosen = jnp.where(start == s, block_ref[:, s * P_SIZE:(s + 2) * P_SIZE], chosen)
    return masked, chosen


def gram_kernel(rows, grp, grows, idx_ref, cnt_ref, sketch_ref, prior_ref, block_ref,
                full_a, full_b, *rest):
    rest = list(rest)
    n = rows * grp
    high, low = rest.pop(0), rest.pop(0)
    plan, gplan = sketch_plan(rows, grp), gram_plan(rows, grp)
    parts = []
    for stages in plan:
        acc = rest.pop(0)
        recvs = [rest.pop(0) for _ in stages]
        parts.append(Halving(stages, acc, recvs, rest.pop(0), rest.pop(0)))
    grams = []
    for stages, full in zip(gplan, (full_a, full_b)):
        acc = rest.pop(0)
        recvs = [rest.pop(0) for _ in stages]
        grams.append(Halving(stages, acc, recvs, *[rest.pop(0) for _ in range(2)], full,
                             *[rest.pop(0) for _ in range(2)]))
    barrier_all(gplan[0])
    masked, chosen = load_columns(idx_ref, cnt_ref, prior_ref, block_ref)
    rh, rl = split(jnp.concatenate([masked, chosen], axis=1))
    sk, width = sketch_ref.shape[0], rh.shape[1]
    per = sk // n
    step = 512
    flat = [[g[0] for g in stages] for stages in plan]
    for lane in range(0, width, 2 * T):
        wide = min(2 * T, width - lane)
        for r in range(0, sk, step):
            if lane == 0:
                h, l = split(sketch_ref[r:r + step, :])
                high[r:r + step, :] = h
                low[r:r + step, :] = l
            pair = (high[r:r + step, :], low[r:r + step, :])
            prod = dot3(pair, (rh[:, lane:lane + wide], rl[:, lane:lane + wide]))
            for j in range(wide // T):
                q = lane // T + j
                spots = block_at(flat[q], flat[0], n)
                for blk in range(r // per, (r + step) // per):
                    s = spots[blk] * per
                    parts[q].acc[s:s + per, :] = prod[blk * per - r:(blk + 1) * per - r, j * T:(j + 1) * T]
        for j in range(wide // T):
            parts[lane // T + j].start(0)
    for i in range(len(plan[0])):
        for part in parts:
            part.finish(i)
            if i + 1 < len(plan[0]):
                part.start(i + 1)
    mine = jnp.concatenate([part.acc[rows_at(part.off, per)] for part in parts], axis=1)
    t = 0
    for i in range(width // T):
        strip = dot(mine[:, i * T:(i + 1) * T], mine[:, :(i + 1) * T], 0, 0)
        for j in range(i + 1):
            q, s = t // 8, (t % 8) * T
            grams[q].acc[s:s + T, :] = strip[:, j * T:(j + 1) * T]
            t += 1
        if t >= 8 and t - i - 1 < 8 and grows == 8 * T:
            grams[0].start(0)
    for q in range(2):
        used = min(8, t - q * 8) * T
        if used < grows:
            grams[q].acc[used:grows, :] = jnp.zeros((grows - used, T), F32)
        if q or grows > 8 * T:
            grams[q].start(0)
    k = len(gplan[0])
    for i in range(k):
        for g in grams:
            g.finish(i)
            if i + 1 < k:
                g.start(i + 1)
            else:
                at = rows_at(g.off, g.size)
                g.full[at] = g.acc[at]
                g.gstart(k - 1)
    for i in range(k - 1, -1, -1):
        for g in grams:
            g.gfinish()
            if i:
                g.gstart(i - 1)


def solve4(tile, p, sides):
    o = p % 8

    def spread(t):
        return [jnp.broadcast_to(t[o + i:o + i + 1, :], (8, T)) for i in range(4)]

    own = spread(tile)

    def at(i, j):
        return jnp.broadcast_to(own[i][:, p + j:p + j + 1], (8, T))

    a, b, e, f = at(0, 0), at(0, 1), at(0, 2), at(0, 3)
    c, g, h = at(1, 1), at(1, 2), at(1, 3)
    x, y, z = at(2, 2), at(2, 3), at(3, 3)
    ra = 1.0 / (a * c - b * b)
    k00, k01 = (c * e - b * g) * ra, (c * f - b * h) * ra
    k10, k11 = (a * g - b * e) * ra, (a * h - b * f) * ra
    s00 = x - (e * k00 + g * k10)
    s01 = y - (e * k01 + g * k11)
    s11 = z - (f * k01 + h * k11)
    rs = 1.0 / (s00 * s11 - s01 * s01)
    out = []
    for side in sides:
        r = spread(side)
        g0, g1 = (c * r[0] - b * r[1]) * ra, (a * r[1] - b * r[0]) * ra
        q2 = r[2] - (k00 * r[0] + k10 * r[1])
        q3 = r[3] - (k01 * r[0] + k11 * r[1])
        n2, n3 = (s11 * q2 - s01 * q3) * rs, (s00 * q3 - s01 * q2) * rs
        out.append([g0 - (k00 * n2 + k01 * n3), g1 - (k10 * n2 + k11 * n3), n2, n3])
    return out


def put4(tile, p, rows):
    sub = lax.broadcasted_iota(jnp.int32, (8, T), 0)
    for j, row in enumerate(rows):
        tile = jnp.where(sub == p % 8 + j, row, tile)
    return tile


def eliminate4(tiles, p):
    v = p // 8
    rows, = solve4(tiles[v], p, [tiles[v]])
    new = []
    for u, w in enumerate(tiles):
        tile = w
        for j in range(4):
            w = w - tile[:, p + j:p + j + 1] * rows[j]
        new.append(put4(w, p, rows) if u == v else w)
    return new


def factor4(mat, low, norm, p):
    v, o = p // 8, p % 8
    sub = lax.broadcasted_iota(jnp.int32, (8, T), 0)
    rows, lows = solve4(mat[v], p, [mat[v], low[v]])
    norm[v] = put4(norm[v], p, lows)
    for u in range(v if o == 0 else v + 1, len(mat)):
        w, l = mat[u], low[u]
        for j in range(4):
            col = jnp.broadcast_to(mat[u][:, p + j:p + j + 1], (8, T))
            w = w - col * rows[j]
            l = l - col * lows[j]
        if u == v:
            w, l = jnp.where(sub >= 4, w, mat[u]), jnp.where(sub >= 4, l, low[u])
        mat[u], low[u] = w, l


def solve_kernel(idx_ref, cnt_ref, prior_ref, block_ref, ta_ref, tb_ref,
                 coef_ref, x_ref, resid_ref, gram_ref, a_ref, inv_ref):
    width = prior_ref.shape[1]
    blocks = width // T + 1
    t = 0
    for i in range(blocks):
        for j in range(i + 1):
            src, s = (ta_ref, t * T) if t < 8 else (tb_ref, (t - 8) * T)
            tile = src[s:s + T, :]
            if i == j and i < blocks - 1:
                row = lax.broadcasted_iota(jnp.int32, (T, T), 0)
                col = lax.broadcasted_iota(jnp.int32, (T, T), 1)
                tile = tile + jnp.where((row == col) & (row + i * T >= cnt_ref[0]), 1.0, 0.0)
            a_ref[i * T:(i + 1) * T, j * T:(j + 1) * T] = tile
            if i != j:
                a_ref[j * T:(j + 1) * T, i * T:(i + 1) * T] = tile.T
            t += 1

    def body(k, _):
        at = pl.ds(pl.multiple_of(k * T, T), T)
        d = a_ref[at, at]
        mat = [d[8 * v:8 * v + 8, :] for v in range(T // 8)]
        lane = lax.broadcasted_iota(jnp.int32, (8, T), 1)
        sub = lax.broadcasted_iota(jnp.int32, (8, T), 0)
        low = [jnp.where(lane == sub + 8 * v, 1.0, 0.0) for v in range(T // 8)]
        norm = [jnp.zeros((8, T), F32) for v in range(T // 8)]
        for p in range(0, T, 4):
            factor4(mat, low, norm, p)
        inv_ref[...] = dot(jnp.concatenate(low, axis=0), jnp.concatenate(norm, axis=0), 0, 0)
        for kk in range(blocks - 1):
            @pl.when(k == kk)
            def _():
                own, rest = slice(kk * T, (kk + 1) * T), slice((kk + 1) * T, blocks * T)
                rowk = dot(inv_ref[...], a_ref[own, rest])
                if kk:
                    top = slice(0, kk * T)
                    a_ref[top, rest] = a_ref[top, rest] - dot(a_ref[top, own], rowk)
                a_ref[rest, rest] = a_ref[rest, rest] - dot(a_ref[rest, own], rowk)
                a_ref[own, rest] = rowk
        return 0

    lax.fori_loop(0, blocks - 1, body, 0)
    coef = a_ref[0:width, width:width + T]
    coef_ref[...] = coef
    e = a_ref[width:width + P_SIZE, width:width + T]
    tiles = [e[8 * v:8 * v + 8, :] for v in range(P_SIZE // 8)]
    for p in range(0, P_SIZE, 4):
        tiles = eliminate4(tiles, p)
    x = jnp.concatenate(tiles, axis=0)[:, P_SIZE:]
    x_ref[...] = x
    masked, chosen = load_columns(idx_ref, cnt_ref, prior_ref, block_ref)
    resid = chosen - dot(masked, coef)
    one = resid[:, :P_SIZE]
    two = resid[:, P_SIZE:] - dot(one, x)
    resid_ref[...] = jnp.concatenate([one, two], axis=1)
    gram_ref[...] = jnp.concatenate([dot(one, one, 0, 0), dot(two, two, 0, 0)], axis=1)


def sum_kernel(rows, grp, gram_ref, out_ref, half, *rest):
    stages = gram_plan(rows, grp)[0]
    core, wide = stages[0], stages[1:]
    slots, holds = rest[:len(wide)], rest[len(wide):2 * len(wide)]
    send_sem, recv_sem = rest[2 * len(wide):]
    barrier_all(stages)
    size = gram_ref.shape[0] // 2
    mine = rows_at(spot_in(core) * size, size)
    c = remote(gram_ref.at[rows_at(spot_in(core, 1) * size, size)], half, send_sem.at[0, 0],
               recv_sem.at[0, 0], core, 1)
    c.start()
    c.wait()
    total = gram_ref[mine, :] + half[...]
    for i, group in enumerate(wide):
        src = holds[i]
        src[...] = total
        here = spot_in(group)
        pend = []
        for m in range(1, 1 << len(group)):
            c = remote(src, slots[i].at[here], send_sem.at[i + 1, m - 1], recv_sem.at[i + 1, m - 1], group, m)
            c.start()
            pend.append(c)
        slots[i][here] = total
        for c in pend:
            c.wait()
        total = slots[i][0]
        for m in range(1, 1 << len(group)):
            total = total + slots[i][m]
    out_ref[mine, :] = total
    k = len(stages)
    c = remote(out_ref.at[mine], out_ref.at[mine], send_sem.at[k, 0], recv_sem.at[k, 0], core, 1)
    c.start()
    c.wait()


def finish_kernel(scale, gram_ref, resid_ref, x_ref, coef_ref, basis_ref, factors_ref):
    gram = gram_ref[...]
    eye = (lax.broadcasted_iota(jnp.int32, (P_SIZE, P_SIZE), 0)
           == lax.broadcasted_iota(jnp.int32, (P_SIZE, P_SIZE), 1)).astype(F32)
    sub = lax.broadcasted_iota(jnp.int32, (8, T), 0)
    mats = []
    for h in range(2):
        m = jnp.concatenate([gram[:, h * P_SIZE:(h + 1) * P_SIZE], eye], axis=1)
        mats.append([m[8 * v:8 * v + 8, :] for v in range(P_SIZE // 8)])
    for p in range(0, P_SIZE, 2):
        v, o = p // 8, p % 8
        for h in range(2):
            tiles = mats[h]
            r0, r1 = (jnp.broadcast_to(tiles[v][o + i:o + i + 1, :], (8, T)) for i in range(2))
            a, b = (jnp.broadcast_to(r0[:, p + i:p + i + 1], (8, T)) for i in range(2))
            c = jnp.broadcast_to(r1[:, p + 1:p + 2], (8, T))
            y0 = lax.rsqrt(a)
            y0 = y0 * (1.5 - 0.5 * a * y0 * y0)
            side = b * y0
            d = c - side * side
            y1 = lax.rsqrt(d)
            y1 = y1 * (1.5 - 0.5 * d * y1 * y1)
            row0 = r0 * y0
            row1 = (r1 - side * row0) * y1
            new = list(tiles)
            for u in range(v, P_SIZE // 8):
                c0 = tiles[u][:, p:p + 1] * y0
                c1 = (tiles[u][:, p + 1:p + 2] - c0 * side) * y1
                w = tiles[u] - c0 * row0 - c1 * row1
                if u == v:
                    w = jnp.where(sub > o + 1, w, tiles[u])
                    w = jnp.where(sub == o, row0, jnp.where(sub == o + 1, row1, w))
                new[u] = w
            mats[h] = new
    full = [jnp.concatenate(m, axis=0) for m in mats]
    row = lax.broadcasted_iota(jnp.int32, (P_SIZE, P_SIZE), 0)
    col = lax.broadcasted_iota(jnp.int32, (P_SIZE, P_SIZE), 1)
    upper = [jnp.where(row <= col, f[:, :P_SIZE], 0.0) for f in full]
    lowinv = [f[:, P_SIZE:] for f in full]
    basis_ref[...] = jnp.concatenate(
        [dot(resid_ref[:, h * P_SIZE:(h + 1) * P_SIZE], lowinv[h], 1, 1) for h in range(2)], axis=1
    ) * scale
    width = coef_ref.shape[0]
    factors_ref[0:width, :] = coef_ref[...]
    inner = dot(upper[0], x_ref[...])
    factors_ref[width:width + P_SIZE, :] = jnp.concatenate([upper[0], inner], axis=1)
    factors_ref[width + P_SIZE:, :] = jnp.concatenate([jnp.zeros_like(eye), upper[1]], axis=1)


def shards(rows, grp, sketch, prior, block, idx, cnt):
    n = rows * grp
    sk, local = sketch.shape
    width = prior.shape[1]
    vm = pl.BlockSpec(memory_space=pltpu.VMEM)
    sm = pl.BlockSpec(memory_space=pltpu.SMEM)
    grows = n * max(8, 8 * T // n)
    scratch = [pltpu.VMEM((sk, local), jnp.bfloat16)] * 2
    for stages in sketch_plan(rows, grp):
        scratch += [pltpu.VMEM((sk, T), F32)] + recv_shapes(stages, sk, T) + [sem_shape(stages)] * 2
    for stages in gram_plan(rows, grp):
        scratch += [pltpu.VMEM((grows, T), F32)] + recv_shapes(stages, grows, T) + [sem_shape(stages)] * 4
    tiles = pl.pallas_call(
        functools.partial(gram_kernel, rows, grp, grows),
        out_shape=[jax.ShapeDtypeStruct((grows, T), F32)] * 2,
        in_specs=[sm, sm, vm, vm, vm],
        out_specs=[vm, vm],
        scratch_shapes=scratch,
        compiler_params=pltpu.CompilerParams(
            collective_id=0, has_side_effects=True, vmem_limit_bytes=VMEM_LIMIT
        ),
    )(idx, cnt, sketch, prior, block)
    coef, x, resid, gram = pl.pallas_call(
        solve_kernel,
        out_shape=[
            jax.ShapeDtypeStruct((width, T), F32),
            jax.ShapeDtypeStruct((P_SIZE, P_SIZE), F32),
            jax.ShapeDtypeStruct((local, T), F32),
            jax.ShapeDtypeStruct((P_SIZE, T), F32),
        ],
        in_specs=[sm, sm, vm, vm, vm, vm],
        out_specs=[vm] * 4,
        scratch_shapes=[pltpu.VMEM((width + T, width + T), F32), pltpu.VMEM((T, T), F32)],
        compiler_params=pltpu.CompilerParams(vmem_limit_bytes=VMEM_LIMIT),
    )(idx, cnt, prior, block, *tiles)
    scale = float(local * n) ** 0.5
    stages = gram_plan(rows, grp)[0]
    half = P_SIZE // 2
    most = max((1 << len(g)) - 1 for g in stages)
    gram = pl.pallas_call(
        functools.partial(sum_kernel, rows, grp),
        out_shape=jax.ShapeDtypeStruct((P_SIZE, T), F32),
        in_specs=[vm],
        out_specs=vm,
        scratch_shapes=[pltpu.VMEM((half, T), F32)]
        + [pltpu.VMEM((1 << len(g), half, T), F32) for g in stages[1:]]
        + [pltpu.VMEM((half, T), F32) for g in stages[1:]]
        + [pltpu.SemaphoreType.DMA((len(stages) + 1, most))] * 2,
        compiler_params=pltpu.CompilerParams(collective_id=1, has_side_effects=True),
    )(gram)
    return tuple(pl.pallas_call(
        functools.partial(finish_kernel, scale),
        out_shape=[
            jax.ShapeDtypeStruct((local, T), F32),
            jax.ShapeDtypeStruct((width + T, T), F32),
        ],
        in_specs=[vm] * 4,
        out_specs=[vm] * 2,
        compiler_params=pltpu.CompilerParams(vmem_limit_bytes=VMEM_LIMIT),
    )(gram, resid, x, coef))


def solution(mesh):
    rows, grp = mesh.shape["rows"], mesh.shape["grp"]
    placed = (
        P(None, ("rows", "grp")),
        P(("rows", "grp"), None),
        P(("rows", "grp"), None),
        P(),
        P(),
    )
    return jax.shard_map(
        functools.partial(shards, rows, grp),
        mesh=mesh,
        in_specs=placed,
        out_specs=(P(("rows", "grp"), None), P()),
        check_vma=False,
    )
```
